32 devices in a mesh: grp: 2 (over x), row: 4 (over y, core), diag: 4 (over z).
Axes of the slice: x: 2, y: 2, z: 4, core: 2. Of those that a mesh axis runs over, the one named last changes fastest.
Arguments:
- emb_rows: bfloat16 [32, 1024], P(None, ('grp', 'row')), parts along dimension 1, may hold values from -6 to 6
- emb_cols: bfloat16 [32, 1024], P(None, ('grp', 'row')), parts along dimension 1, may hold values from -6 to 6
- kernel: bfloat16 [3, 3, 32, 32], replicated, may hold values from -0.375 to 0.375
- bias: float32 [32], replicated, may hold values from -3 to 3
- cotangent: bfloat16 [32, 1024, 512], P(None, ('grp', 'row'), 'diag'), parts along dimension 1, may hold values from -6 to 6
- valid: int32 [1024], P(('grp', 'row')), parts along dimension 0, may hold values 0 or 1
- dilation: int32 [2], P('grp'), parts along dimension 0, may hold values from 1 to 4
- band: int32 [2], P('grp'), parts along dimension 0, may hold values from 384 to 512
Outputs:
- pair_out: bfloat16 [32, 1024, 512], P(None, ('grp', 'row'), 'diag'), parts along dimension 1
- row_grad: float32 [32, 1024], P(None, ('grp', 'row')), parts along dimension 1
- col_grad: float32 [32, 1024], P(None, ('grp', 'row')), parts along dimension 1
- kernel_grad: float32 [6, 3, 32, 32], P('grp'), parts along dimension 0
- bias_grad: float32 [64], P('grp'), parts along dimension 0
The draws below stay inside these ranges and needn't reach their ends.
There are 2 independent parts, one for each index of `grp`. The reference program is written for one: setup_inputs(seed, part) draws one part's arguments, and reference() takes and returns one part's arrays. A program takes and returns all parts, laid end to end along the dimension named above; an argument that names none is the same for every part. Nothing has to cross between parts.
All inputs are finite; a program needn't handle non-finite values. No bound on the sum of `valid` on one device may be relied on, other than what follows from the above.
Results may differ from the reference program's by a relative error of at most 0.0032.
Values may be sent and summed in bfloat16 or wider, within the bound.
No kernel may reach another device: no remote copies, remote signals or barrier semaphores. Data moves between devices by JAX's collectives and lax.ppermute only.
A program may use at most 128 MiB of HBM per device.

```python
import jax
import jax.numpy as jnp
from jax import lax

CH = 32
MAXDIL = 4
ROWS_DEV = 128
LENGTH = 512
DIAGONAL_COUNT = 512


def touch_ends(drawn, stream_key, low, high):
    spot = [jax.random.randint(jax.random.fold_in(stream_key, axis), (), 0, length) for axis, length in enumerate(drawn.shape)]
    widest = drawn.shape.index(max(drawn.shape))
    neighbour = spot[:widest] + [(spot[widest] + 1) % drawn.shape[widest]] + spot[widest + 1:]
    return drawn.at[tuple(spot)].set(low).at[tuple(neighbour)].set(high)


def steps_of(rng, extent, cuts, low, top_value):
    level, own = 1.0, jax.random.fold_in(rng, 6)
    for dim, shards_of in cuts:
        draws = jnp.exp(jax.random.uniform(jax.random.fold_in(own, dim), (shards_of,), jnp.float32, low / len(cuts), top_value / len(cuts)))
        level = level * jnp.repeat(draws, extent[dim] // shards_of).reshape([-1 if axis == dim else 1 for axis in range(len(extent))])
    return level


def scatter_about(own_key, extent, deviation, limit, split=(), held_as=jnp.bfloat16):
    values = jax.random.normal(own_key, extent, jnp.float32) * deviation
    if len(split) > 0:
        values = steps_of(own_key, extent, split, -0.22, 0.18) * values
    return jnp.clip(values, min=-limit, max=limit).astype(held_as)


def setup_inputs(seed: int = 0, part: int = 0) -> dict:
    arg_keys = jax.random.split(jax.random.key(seed), 9)
    own_keys = jax.random.split(jax.random.fold_in(arg_keys[8], part), 9)
    return {
        "emb_rows": scatter_about(own_keys[0], (CH, LENGTH), 1.0, 6.0, ((1, 4),)),
        "emb_cols": scatter_about(own_keys[1], (CH, LENGTH), 1.0, 6.0, ((1, 4),)),
        "kernel": scatter_about(arg_keys[2], (3, 3, CH, CH), (9 * CH) ** -0.5, 0.375),
        "bias": scatter_about(arg_keys[3], (CH,), 0.5, 3.0, (), jnp.float32),
        "cotangent": scatter_about(own_keys[4], (CH, LENGTH, DIAGONAL_COUNT), 1.0, 6.0, ((1, 4), (2, 4))),
        "valid": touch_ends((jax.random.randint(own_keys[5], (LENGTH,), 0, 10) < 9).astype(jnp.int32), jax.random.fold_in(own_keys[5], 1), 0, 1),
        "dilation": jax.random.randint(own_keys[6], (1,), 1, MAXDIL + 1).astype(jnp.int32),
        "band": jax.random.randint(own_keys[7], (1,), DIAGONAL_COUNT * 3 // 4, DIAGONAL_COUNT + 1).astype(jnp.int32),
    }


def diagonal_take(window, row_number, diagonal_number):
    span_width = row_number + diagonal_number - 1
    leading = window.shape[:-1]
    widened = jnp.broadcast_to(window[..., None, :], leading + (row_number, span_width))
    flattened = widened.reshape(leading + (row_number * span_width,))
    flattened = jnp.pad(flattened, [(0, 0)] * len(leading) + [(0, row_number)])
    return flattened.reshape(leading + (row_number, span_width + 1))[..., :diagonal_number]

def diagonal_fold(field):
    channels, row_number, diagonal_number = field.shape
    span_width = row_number + diagonal_number - 1
    padded = jnp.pad(field, ((0, 0), (0, 0), (0, span_width + 1 - diagonal_number)))
    flattened = padded.reshape(channels, row_number * (span_width + 1))[:, :row_number * span_width]
    return lax.optimization_barrier(jnp.sum(flattened.reshape(channels, row_number, span_width), axis=1))

def diagonal_sums(field):
    channels, row_number, diagonal_number = field.shape
    block_row_list = 128 if row_number % 128 == 0 else row_number
    part_width = block_row_list + diagonal_number - 1

    def accumulate(index, totals):
        first = index * block_row_list
        piece = lax.dynamic_slice_in_dim(field, first, block_row_list, 1)
        current = lax.dynamic_slice_in_dim(totals, first, part_width, 1)
        return lax.dynamic_update_slice_in_dim(totals, current + diagonal_fold(piece), first, 1)
    totals = jnp.zeros((channels, row_number + diagonal_number - 1), jnp.float32)
    return lax.fori_loop(0, row_number // block_row_list, accumulate, totals)

def pair_block(row_embed, row_valid, col_window, col_valid, first_diag, row_number, diagonal_number, band_limit):
    outer = row_embed.astype(jnp.float32)[:, :, None] + diagonal_take(col_window, row_number, diagonal_number).astype(jnp.float32)
    offsets = first_diag + jnp.arange(diagonal_number, dtype=jnp.int32)
    inside = ((offsets >= 0) & (offsets < band_limit)).astype(jnp.float32)
    validity = row_valid[:, None] * diagonal_take(col_valid[None], row_number, diagonal_number)[0] * inside[None, :]
    hidden = outer * validity
    active = (jax.nn.gelu(hidden) * validity).astype(jnp.bfloat16)
    return (hidden, validity, active)

def contract(form, left, right):
    return jnp.einsum(form, left.astype(jnp.float32), right.astype(jnp.float32))

def dilated_convolve(active_extended, kernel, dilation_factor, row_number, diagonal_number, border_width):
    channels = active_extended.shape[0]
    result = jnp.zeros((kernel.shape[2], row_number, diagonal_number), jnp.float32)
    for kernel_tap_row in range(3):
        for kernel_tap_column in range(3):
            corner_patch = (jnp.int32(0), border_width + (kernel_tap_row - 1) * dilation_factor, border_width + (kernel_tap_column - kernel_tap_row) * dilation_factor)
            piece = lax.dynamic_slice(active_extended, corner_patch, (channels, row_number, diagonal_number))
            result = result + contract('oc,crk->ork', kernel[kernel_tap_row, kernel_tap_column], piece)
    return result

def kernel_summands(gradient_local, active_extended, dilation_factor, row_number, diagonal_number, border_width):
    channels = active_extended.shape[0]
    taps = []
    for kernel_tap_row in range(3):
        for kernel_tap_column in range(3):
            corner_patch = (jnp.int32(0), border_width + (kernel_tap_row - 1) * dilation_factor, border_width + (kernel_tap_column - kernel_tap_row) * dilation_factor)
            piece = lax.dynamic_slice(active_extended, corner_patch, (channels, row_number, diagonal_number))
            taps.append(contract('ork,crk->oc', gradient_local, piece))
    return jnp.stack(taps).reshape(3, 3, channels, channels)

def dilated_convolve_grad(gradient_extended, kernel, dilation_factor, row_number, diagonal_number, border_width):
    channels = gradient_extended.shape[0]
    result = jnp.zeros((kernel.shape[3], row_number, diagonal_number), jnp.float32)
    for kernel_tap_row in range(3):
        for kernel_tap_column in range(3):
            corner_patch = (jnp.int32(0), border_width - (kernel_tap_row - 1) * dilation_factor, border_width - (kernel_tap_column - kernel_tap_row) * dilation_factor)
            piece = lax.dynamic_slice(gradient_extended, corner_patch, (channels, row_number, diagonal_number))
            result = result + contract('oc,ork->crk', kernel[kernel_tap_row, kernel_tap_column], piece)
    return result

def reference(emb_rows, emb_cols, kernel, bias, cotangent, valid, dilation, band):
    border_width = 2 * MAXDIL
    block_row_list = ROWS_DEV
    channels = emb_rows.shape[0]
    dilation_factor = dilation[0]
    band_limit = band[0]
    valid_float = valid.astype(jnp.float32)
    cols_padded = jnp.pad(emb_cols, ((0, 0), (2 * border_width, DIAGONAL_COUNT + 2 * border_width + block_row_list)))
    cvalid_padded = jnp.pad(valid_float, (2 * border_width, DIAGONAL_COUNT + 2 * border_width + block_row_list))
    rows_padded = jnp.pad(emb_rows, ((0, 0), (border_width, border_width)))
    rvalid_padded = jnp.pad(valid_float, (border_width, border_width))
    grad_padded = jnp.pad(cotangent, ((0, 0), (border_width, border_width), (border_width, border_width)))

    def advance(carry, block_index):
        col_totals, kernel_total, bias_total = carry
        first = block_index * block_row_list
        row_embed = lax.dynamic_slice_in_dim(rows_padded, first, block_row_list + 2 * border_width, 1)
        row_valid = lax.dynamic_slice_in_dim(rvalid_padded, first, block_row_list + 2 * border_width, 0)
        span = block_row_list + DIAGONAL_COUNT + 4 * border_width - 1
        col_window = lax.dynamic_slice_in_dim(cols_padded, first, span, 1)
        col_valid = lax.dynamic_slice_in_dim(cvalid_padded, first, span, 0)
        hidden_ext, valid_ext, active_extended = pair_block(row_embed, row_valid, col_window, col_valid, -border_width, block_row_list + 2 * border_width, DIAGONAL_COUNT + 2 * border_width, band_limit)
        hidden = hidden_ext[:, border_width:border_width + block_row_list, border_width:border_width + DIAGONAL_COUNT]
        validity = valid_ext[border_width:border_width + block_row_list, border_width:border_width + DIAGONAL_COUNT]
        mixed_features = dilated_convolve(active_extended, kernel, dilation_factor, block_row_list, DIAGONAL_COUNT, border_width) + bias[:, None, None]
        output = ((hidden + mixed_features) * validity).astype(jnp.bfloat16)
        corner_patch = (jnp.int32(0), first, jnp.int32(0))
        grad_window = lax.dynamic_slice(grad_padded, corner_patch, (channels, block_row_list + 2 * border_width, DIAGONAL_COUNT + 2 * border_width))
        gradient_extended = (grad_window.astype(jnp.float32) * valid_ext).astype(jnp.bfloat16)
        gradient_local = gradient_extended[:, border_width:border_width + block_row_list, border_width:border_width + DIAGONAL_COUNT]
        kernel_portion = kernel_summands(gradient_local, active_extended, dilation_factor, block_row_list, DIAGONAL_COUNT, border_width)
        bias_part = lax.optimization_barrier(jnp.sum(gradient_local.astype(jnp.float32), axis=(1, 2)))
        activation_grad = dilated_convolve_grad(gradient_extended, kernel, dilation_factor, block_row_list, DIAGONAL_COUNT, border_width)
        unused, pullback = jax.vjp(jax.nn.gelu, hidden)
        dpair = (gradient_local.astype(jnp.float32) + pullback(activation_grad * validity)[0]) * validity
        row_part = lax.optimization_barrier(jnp.sum(dpair, axis=2))
        col_part = diagonal_sums(dpair)
        current = lax.dynamic_slice_in_dim(col_totals, first, block_row_list + DIAGONAL_COUNT - 1, 1)
        col_totals = lax.dynamic_update_slice_in_dim(col_totals, current + col_part, first, 1)
        return ((col_totals, kernel_total + kernel_portion, bias_total + bias_part), (output, row_part))
    start = (jnp.zeros((channels, LENGTH + DIAGONAL_COUNT + block_row_list), jnp.float32), jnp.zeros((3, 3, channels, channels), jnp.float32), jnp.zeros((channels,), jnp.float32))
    count = LENGTH // block_row_list
    final, stacked = lax.scan(advance, start, jnp.arange(count, dtype=jnp.int32))
    col_totals, kernel_total, bias_total = final
    outputs, row_parts = stacked
    pair_out = jnp.transpose(outputs, (1, 0, 2, 3)).reshape(channels, LENGTH, DIAGONAL_COUNT)
    row_sum = jnp.transpose(row_parts, (1, 0, 2)).reshape(channels, LENGTH)
    embed_scale = 1.0 / jnp.sqrt(jnp.float32(DIAGONAL_COUNT))
    weight_scale = 1.0 / jnp.sqrt(jnp.float32(LENGTH) * jnp.float32(DIAGONAL_COUNT))
    return (pair_out, row_sum * embed_scale, col_totals[:, :LENGTH] * embed_scale, kernel_total * weight_scale, bias_total * weight_scale)
```

```python
import jax
import jax.numpy as jnp
from jax import lax
from jax.experimental import pallas as pl
from jax.experimental.pallas import tpu as pltpu
from jax.sharding import PartitionSpec as P

MAXDIL = 4
EDGE = 2 * MAXDIL
SLOT = 2 * EDGE
GELU_C = 0.7978845608028654
GELU_A = 0.044715


def gelu_and_slope(h):
    square = h * h
    t = jnp.tanh(h * (GELU_C + (GELU_C * GELU_A) * square))
    half = 0.5 * h
    one = 1.0 + t
    slope = 0.5 * one + half * (1.0 - t * t) * (GELU_C + (3.0 * GELU_C * GELU_A) * square)
    return half * one, slope


def tile_kernel(
    gathered, kernel, bias, cot, dil, band,
    pair_out, sums, kgrad,
    act_halo, taps, gtaps, hid, slope, vmask, gz, gedge, cols, colv, accs, kacc,
):
    ch = bias.shape[0]
    n = cot.shape[1]
    sub = ch // 8
    blocks = gathered.shape[0]
    extra = MAXDIL
    ext = n + 2 * extra
    packs = ext
    xhalo = ext + SLOT
    r_id = lax.axis_index("row")
    k_id = lax.axis_index("diag")
    r = dil[0]
    width = band[0] - k_id * n
    low = -k_id * n
    f32, bf16 = jnp.float32, jnp.bfloat16
    lane8 = lax.broadcasted_iota(jnp.int32, (8, n), 1)
    lane16 = lax.broadcasted_iota(jnp.int32, (16, n), 1)
    lim = {s: (s * r).astype(f32).astype(bf16) for s in (1, 2, -1, -2)}
    top = {s: (n - s * r).astype(f32).astype(bf16) for s in (1, 2)}

    def block_of(index, first, count):
        found = gathered[jnp.clip(index, 0, blocks - 1), first : first + count, :]
        inside = ((index >= 0) & (index < blocks)).astype(f32)
        return found.astype(f32) * inside

    for t in range(4):
        cols[t] = block_of(r_id + k_id + t - 1, 0, ch).reshape(sub, 8, n)
        colv[t] = block_of(r_id + k_id + t - 1, 2 * ch, 8)

    def row_values(index):
        return block_of(index, ch, ch), block_of(index, 2 * ch, 8)

    own, own_v = row_values(r_id)
    prev, prev_v = row_values(r_id - 1)
    nxt, nxt_v = row_values(r_id + 1)

    def unit(slot, rows, rows_v, col, col_v, inside):
        v = jnp.where(inside, rows_v * col_v, 0.0)
        h = (rows + col) * v[None]
        a, g = gelu_and_slope(h)
        slope[slot] = g * v[None]
        vmask[slot] = jnp.concatenate([v, v], axis=0).astype(bf16)
        return h, a.reshape(ch, n).astype(bf16)

    def spread(rows, at):
        return jnp.broadcast_to(rows[:, at : at + 1], rows.shape)

    def pick(t):
        col, col_v = cols[3], colv[3]
        for b in (2, 1, 0):
            here = t == b - 1
            col = jnp.where(here[None], cols[b], col)
            col_v = jnp.where(here, colv[b], col_v)
        return col, col_v

    for p in range(SLOT):
        loose = p + SLOT * ((lane8 - p + EDGE) >> 4)
        row = loose & (n - 1)
        e = lane8 - loose
        d = jnp.where(e < 0, e, e + n)
        col, col_v = pick((row + d) >> 7)
        index = jnp.concatenate([row] * sub, axis=0)
        rows = jnp.take_along_axis(own, index, axis=1).reshape(sub, 8, n)
        rows_v = jnp.take_along_axis(own_v, row, axis=1)
        _, a = unit(packs + p, rows, rows_v, col, col_v, (d >= low) & (d < width))
        act_halo[p] = a

    lane32 = lax.broadcasted_iota(jnp.int32, (ch, n), 1)
    near = jnp.where(lane32 < extra, pltpu.roll(prev, extra, 1), pltpu.roll(nxt, extra, 1))
    near_v = jnp.where(lane8 < extra, pltpu.roll(prev_v, extra, 1), pltpu.roll(nxt_v, extra, 1))
    near_rows = [y - extra if y < extra else n + y - extra for y in range(2 * extra)]
    for y, i in enumerate(near_rows):
        e = ((lane8 - i + EDGE) & (n - 1)) - EDGE
        d = jnp.where(e < 0, e, e + n)
        rows = spread(near, y).reshape(sub, 8, n)
        rows_v = spread(near_v, y)
        col, col_v = pick((i + d) >> 7)
        inside = (e < EDGE) & (d >= low) & (d < width)
        _, a = unit(xhalo + y, rows, rows_v, col, col_v, inside)
        act_halo[SLOT + y] = a

    def store_taps(i, a, halo):
        d = ((lane16 - i) & (n - 1)).astype(f32).astype(bf16)
        a2, h2 = a.reshape(2, 16, n), halo.reshape(2, 16, n)

        def sel(mask):
            return jnp.where(mask[None], h2, a2).reshape(ch, n)

        up1, up2 = sel(d < lim[1]), sel(d < lim[2])
        dn1, dn2 = sel(d >= top[1]), sel(d >= top[2])
        byshift = {0: a, 1: up1, 2: up2, -1: dn1, -2: dn2}
        back = n - r
        for ta in range(3):
            at = i - (ta - 1) * r + EDGE
            for tb in range(3):
                x = byshift[tb - ta]
                if tb == 0:
                    x = pltpu.roll(x, r, 1)
                elif tb == 2:
                    x = pltpu.roll(x, back, 1)
                tap = (3 * ta + tb) * ch
                taps[at, tap : tap + ch, :] = x

    for y, i in enumerate(near_rows):
        d = (lane8 - i) & (n - 1)
        rows = spread(near, y).reshape(sub, 8, n)
        rows_v = spread(near_v, y)
        col, col_v = pick((i + d) >> 7)
        _, a = unit(i + extra, rows, rows_v, col, col_v, (d >= low) & (d < width))
        store_taps(i, a, act_halo[SLOT + y])

    group = 8

    def rows_step(g, carry):
        base = g * group
        turned = pltpu.roll(own, (n - base) & (n - 1), 1)
        turned_v = pltpu.roll(own_v, (n - base) & (n - 1), 1)
        for u in range(group):
            i = base + u
            here = lane8 >= i
            col = jnp.where(here[None], cols[1], cols[2])
            col_v = jnp.where(here, colv[1], colv[2])
            d = (lane8 - i) & (n - 1)
            rows = spread(turned, u).reshape(sub, 8, n)
            h, a = unit(i + extra, rows, spread(turned_v, u), col, col_v, (d >= low) & (d < width))
            hid[i] = h
            store_taps(i, a, act_halo[i & (SLOT - 1)])
        return carry

    lax.fori_loop(0, n // group, rows_step, 0)

    for at in list(range(2 * extra)) + list(range(n, ext)) + list(range(xhalo, xhalo + 2 * extra)):
        gtaps[at] = jnp.zeros(gtaps.shape[1:], bf16)
    gedge[...] = jnp.zeros(gedge.shape, bf16)

    def turn(x, tb):
        if tb == 0:
            return pltpu.roll(x, n - r, 1)
        if tb == 2:
            return pltpu.roll(x, r, 1)
        return x

    def keep(x, mask):
        x2 = x.reshape(2, 16, n)
        return jnp.where(mask[None], x2, jnp.zeros_like(x2)).reshape(ch, n)

    def grads_step(g, carry):
        base = pl.multiple_of(g * 16, 16)
        block = jnp.swapaxes(cot[:, pl.ds(base, 16), :], 0, 1)
        for u in range(16):
            i = base + u
            x = pltpu.roll(block[u], i, 1)
            x = (x.reshape(2, 16, n) * vmask[i + extra][None]).reshape(ch, n)
            gz[i] = x
            d = ((lane16 - i) & (n - 1)).astype(f32).astype(bf16)
            slot = ((lane16 - i + EDGE) & (n - 1)).astype(f32).astype(bf16)
            old = gedge[u].reshape(2, 16, n)
            gedge[u] = jnp.where(
                (slot < jnp.array(SLOT, bf16))[None], x.reshape(2, 16, n), old
            ).reshape(ch, n)
            byshift = {0: x}
            for s in (1, 2):
                byshift[s] = keep(x, d < top[s])
                byshift[-s] = keep(x, d >= lim[s])
            for ta in range(3):
                at = i + (ta - 1) * r + extra
                for tb in range(3):
                    tap = (3 * ta + tb) * ch
                    gtaps[at, tap : tap + ch, :] = turn(byshift[tb - ta], tb)
        return carry

    lax.fori_loop(0, n // 16, grads_step, 0)

    for p in range(SLOT):
        loose = p + SLOT * ((lane16 - p + EDGE) >> 4)
        row = (loose & (n - 1)).astype(f32).astype(bf16)
        e = (lane16 - loose).astype(f32).astype(bf16)
        x = gedge[p]
        zero = jnp.array(0, bf16)
        for ta in range(3):
            at = packs + ((p + (ta - 1) * r) & (SLOT - 1))
            for tb in range(3):
                s = tb - ta
                tap = (3 * ta + tb) * ch
                if s == 0:
                    gtaps[at, tap : tap + ch, :] = jnp.zeros((ch, n), bf16)
                    continue
                if s > 0:
                    mask = (e < zero) & (e >= lim[-s])
                else:
                    mask = (e >= zero) & (e < lim[-s])
                if ta == 0:
                    mask = mask & (row >= lim[1])
                elif ta == 2:
                    mask = mask & (row < top[1])
                gtaps[at, tap : tap + ch, :] = turn(keep(x, mask), tb)

    for y in range(extra):
        for ta, i in ((0, y), (2, n - 1 - y)):

            @pl.when(r > y)
            def _(ta=ta, i=i):
                x = gz[i]
                d = ((lane16 - i) & (n - 1)).astype(f32).astype(bf16)
                at = xhalo + (i - r + extra if ta == 0 else extra + i + r - n)
                for tb in range(3):
                    s = tb - ta
                    if s == 0:
                        continue
                    mask = d >= top[s] if s > 0 else d < lim[-s]
                    tap = (3 * ta + tb) * ch
                    gtaps[at, tap : tap + ch, :] = turn(keep(x, mask), tb)

    taps_w = [kernel[t // 3, t % 3] for t in range(9)]
    w_out = jnp.concatenate(taps_w, axis=1)
    w_in = jnp.concatenate([w.astype(f32).T.astype(bf16) for w in taps_w], axis=1)
    kacc[...] = jnp.zeros(kacc.shape, f32)
    shift_by = jnp.broadcast_to(bias[...], (ch, n))

    def conv_step(g, carry):
        base = pl.multiple_of(g * 16, 16)
        done = []
        total = None
        for u in range(0, 16, 2):
            i = base + u
            both = jnp.concatenate([taps[i + EDGE], taps[i + EDGE + 1]], axis=1)
            grads = jnp.concatenate([gz[i], gz[i + 1]], axis=1)
            z = jnp.dot(w_out, both, preferred_element_type=f32)
            part = lax.dot_general(
                both, grads, (((1,), (1,)), ((), ())), preferred_element_type=f32
            )
            total = part if total is None else total + part
            for w in range(2):
                v = vmask[i + w + extra].astype(f32)[:8]
                y = hid[i + w] + (z[:, w * n : (w + 1) * n] + shift_by).reshape(sub, 8, n)
                y = (y * v[None]).reshape(ch, n).astype(bf16)
                done.append(pltpu.roll(y, (n - i - w) & (n - 1), 1))
        kacc[...] += total
        pair_out[:, pl.ds(base, 16), :] = jnp.swapaxes(jnp.stack(done), 0, 1)
        return carry

    lax.fori_loop(0, n // 16, conv_step, 0)

    accs[...] = jnp.zeros(accs.shape, f32)

    def spreads(at):
        both = jnp.concatenate([gtaps[at], gtaps[at + 1]], axis=1)
        da = jnp.dot(w_in, both, preferred_element_type=f32)
        return [
            slope[at + w] * da[:, w * n : (w + 1) * n].reshape(sub, 8, n) for w in range(2)
        ]

    def back_step(g, carry):
        base = g * group
        racc, c0, c1, bacc = accs[1], accs[4], accs[5], accs[7]
        for u in range(0, group, 2):
            i = base + u
            for w, dx in enumerate(spreads(i + extra)):
                gg = gz[i + w].astype(f32).reshape(sub, 8, n)
                bacc = bacc + gg
                dx = dx + gg
                racc = racc + jnp.where(
                    (lane8 == i + w)[None], jnp.sum(dx, axis=2, keepdims=True), 0.0
                )
                here = (lane8 >= i + w)[None]
                c0 = c0 + jnp.where(here, dx, 0.0)
                c1 = c1 + jnp.where(here, 0.0, dx)
        accs[1], accs[4], accs[5], accs[7] = racc, c0, c1, bacc
        return carry

    lax.fori_loop(0, n // group, back_step, 0)

    def add_columns(dx, t):
        for b in range(4):
            accs[3 + b] += jnp.where((t == b - 1)[None], dx, 0.0)

    for y in range(0, 2 * extra, 2):
        i0 = near_rows[y]
        for w, dx in enumerate(spreads(i0 + extra)):
            i = i0 + w
            add_columns(dx, (i + ((lane8 - i) & (n - 1))) >> 7)
            total = jnp.sum(dx, axis=2, keepdims=True)
            accs[0 if y < extra else 2] += jnp.where((lane8 == (i & (n - 1)))[None], total, 0.0)
        for w, dx in enumerate(spreads(xhalo + y)):
            i = i0 + w
            e = ((lane8 - i + EDGE) & (n - 1)) - EDGE
            d = jnp.where(e < 0, e, e + n)
            add_columns(dx, (i + d) >> 7)
            total = jnp.sum(dx, axis=2, keepdims=True)
            accs[0 if y < extra else 2] += jnp.where((lane8 == (i & (n - 1)))[None], total, 0.0)
    for p in range(0, SLOT, 2):
        for w, dx in enumerate(spreads(packs + p)):
            q = p + w
            loose = q + SLOT * ((lane8 - q + EDGE) >> 4)
            e = lane8 - loose
            d = jnp.where(e < 0, e, e + n)
            add_columns(dx, ((loose & (n - 1)) + d) >> 7)
            x = dx.reshape(ch, n)
            for step in (1, 2, 4, 8):
                x = x + pltpu.roll(x, n - step, 1)
            x = pltpu.roll(x, EDGE, 1).reshape(sub, 8, n)
            accs[1] += jnp.where(((lane8 & (SLOT - 1)) == q)[None], x, 0.0)

    sums[...] = jnp.zeros(sums.shape, f32)
    for t in range(3):
        at = r_id + t - 1

        @pl.when((at >= 0) & (at < blocks))
        def _(at=at, t=t):
            sums[at, :ch, :] = accs[t].reshape(ch, n)

    for t in range(4):
        at = r_id + k_id + t - 1

        @pl.when((at >= 0) & (at < blocks))
        def _(at=at, t=t):
            sums[at, ch:, :] = accs[3 + t].reshape(ch, n)

    full = jnp.concatenate(
        [kacc[...].T, jnp.zeros((ch, 3 * n - 9 * ch), f32)], axis=1
    )
    lanes = lax.broadcasted_iota(jnp.int32, (ch, 3 * n), 1)
    btotal = jnp.sum(accs[7].reshape(ch, n), axis=1, keepdims=True)
    full = jnp.where(lanes == 9 * ch, btotal, full)
    for t in range(3):
        kgrad[t * ch : (t + 1) * ch, :] = full[:, t * n : (t + 1) * n]


def tile_call(gathered, kernel, bias, cot, dil, band):
    blocks, _, n = gathered.shape
    ch = bias.shape[0]
    sub = ch // 8
    f32, bf16 = jnp.float32, jnp.bfloat16
    vmem = pl.BlockSpec(memory_space=pltpu.VMEM)
    smem = pl.BlockSpec(memory_space=pltpu.SMEM)
    units = n + 4 * MAXDIL + SLOT
    return pl.pallas_call(
        tile_kernel,
        out_shape=(
            jax.ShapeDtypeStruct((ch, n, n), bf16),
            jax.ShapeDtypeStruct((blocks, 2 * ch, n), f32),
            jax.ShapeDtypeStruct((3 * ch, n), f32),
        ),
        in_specs=[vmem, vmem, vmem, vmem, smem, smem],
        out_specs=(vmem, vmem, vmem),
        scratch_shapes=[
            pltpu.VMEM((SLOT + 2 * MAXDIL, ch, n), bf16),
            pltpu.VMEM((n + 2 * EDGE, 9 * ch, n), bf16),
            pltpu.VMEM((units, 9 * ch, n), bf16),
            pltpu.VMEM((n, sub, 8, n), f32),
            pltpu.VMEM((units, sub, 8, n), f32),
            pltpu.VMEM((units, 16, n), bf16),
            pltpu.VMEM((n, ch, n), bf16),
            pltpu.VMEM((SLOT, ch, n), bf16),
            pltpu.VMEM((4, sub, 8, n), f32),
            pltpu.VMEM((4, 8, n), f32),
            pltpu.VMEM((8, sub, 8, n), f32),
            pltpu.VMEM((9 * ch, ch), f32),
        ],
        compiler_params=pltpu.CompilerParams(vmem_limit_bytes=60 * 1024 * 1024),
    )(gathered, kernel, bias.reshape(ch, 1), cot, dil, band)


def swapped(value, axis, bit):
    return lax.ppermute(value, axis, [(i, i ^ bit) for i in range(lax.axis_size(axis))])


def local(emb_rows, emb_cols, kernel, bias, cotangent, valid, dilation, band):
    ch, n = emb_rows.shape
    row_devices, diag_devices = lax.axis_size("row"), lax.axis_size("diag")
    assert cotangent.shape[2] == n == 128
    assert row_devices & (row_devices - 1) == 0 and diag_devices & (diag_devices - 1) == 0
    total_diags = n * diag_devices
    known = jnp.broadcast_to(valid.astype(jnp.bfloat16)[None], (16, n))
    bins = jnp.concatenate([emb_cols, emb_rows, known], axis=0)
    gathered = lax.all_gather(bins, "row")
    pair_out, sums, kgrad = tile_call(gathered, kernel, bias, cotangent, dilation, band)

    place = lax.axis_index("row")
    bit = row_devices // 2
    while bit:
        halves = sums.reshape((2, bit) + sums.shape[1:])
        mine = (place // bit) & 1
        kept = lax.dynamic_index_in_dim(halves, mine, 0, False)
        sent = lax.dynamic_index_in_dim(halves, 1 - mine, 0, False)
        came = swapped(jnp.concatenate([sent.reshape(-1, n), kgrad], axis=0), "row", bit)
        sums = kept + came[: bit * 2 * ch].reshape(kept.shape)
        kgrad = kgrad + came[bit * 2 * ch :]
        bit //= 2
    both = jnp.concatenate([sums.reshape(2 * ch, n), kgrad], axis=0)
    bit = 1
    while bit < diag_devices:
        both = both + swapped(both, "diag", bit)
        bit *= 2
    embed_scale = 1.0 / jnp.sqrt(jnp.float32(total_diags))
    weight_scale = 1.0 / jnp.sqrt(jnp.float32(row_devices * n) * jnp.float32(total_diags))
    wide = both[2 * ch :].reshape(3, ch, n).transpose(1, 0, 2).reshape(ch, 3 * n)
    kernel_grad = wide[:, : 9 * ch].reshape(ch, 9, ch).transpose(1, 0, 2).reshape(3, 3, ch, ch)
    return (
        pair_out,
        both[:ch] * embed_scale,
        both[ch : 2 * ch] * embed_scale,
        kernel_grad * weight_scale,
        wide[:, 9 * ch] * weight_scale,
    )


def solution(mesh):
    in_specs = (
        P(None, ("grp", "row")),
        P(None, ("grp", "row")),
        P(),
        P(),
        P(None, ("grp", "row"), "diag"),
        P(("grp", "row")),
        P("grp"),
        P("grp"),
    )
    out_specs = (
        P(None, ("grp", "row"), "diag"),
        P(None, ("grp", "row")),
        P(None, ("grp", "row")),
        P("grp", None, None, None),
        P("grp"),
    )
    return jax.shard_map(local, mesh=mesh, in_specs=in_specs, out_specs=out_specs, check_vma=False)
```

```python
import jax
import jax.numpy as jnp
from jax import lax
from jax.experimental import pallas as pl
from jax.experimental.pallas import tpu as pltpu
from jax.sharding import PartitionSpec as P

MAXDIL = 4
EDGE = 2 * MAXDIL
SLOT = 2 * EDGE
GELU_C = 0.7978845608028654
GELU_A = 0.044715
WORD_BITS = 6
VMEM_LIMIT = (65472 - 900) * 1024
OUT_LIMIT = (65472 - 1500) * 1024


def gelu_and_slope(h):
    square = h * h
    t = jnp.tanh(h * (GELU_C + (GELU_C * GELU_A) * square))
    half = 0.5 * h
    one = 1.0 + t
    slope = 0.5 * one + half * (1.0 - t * t) * (GELU_C + (3.0 * GELU_C * GELU_A) * square)
    return half * one, slope


def crossings():
    return [(ta, tb) for ta in range(3) for tb in range(3) if ta != tb]


def pack_kernel(emb_cols, emb_rows, valid, dil, band, kernel, bins, weights):
    f32, bf16 = jnp.float32, jnp.bfloat16
    ch, n = emb_cols.shape
    bins[:ch] = emb_cols[...]
    bins[ch : 2 * ch] = emb_rows[...]
    known = jnp.broadcast_to(valid[...].astype(f32), (8, n))
    wide = jnp.broadcast_to(band[...], (8, n))
    line = lax.broadcasted_iota(jnp.int32, (8, n), 0)
    settings = jnp.where(line == 1, wide >> WORD_BITS, wide & (2**WORD_BITS - 1))
    settings = jnp.where(line == 0, jnp.broadcast_to(dil[...], (8, n)), settings)
    bins[2 * ch :] = jnp.concatenate([known, settings.astype(f32)], axis=0).astype(bf16)
    taps = [kernel[t // 3, t % 3] for t in range(9)]
    turned = [w.astype(f32).T.astype(bf16) for w in taps]
    cross = [3 * ta + tb for ta, tb in crossings()]
    weights[0] = jnp.concatenate(taps, axis=1)
    weights[1] = jnp.concatenate(turned, axis=1)
    weights[2, :, : 6 * ch] = jnp.concatenate([taps[t] for t in cross], axis=1)
    weights[3, :, : 6 * ch] = jnp.concatenate([turned[t] for t in cross], axis=1)


def pack_call(emb_cols, emb_rows, valid, dil, band, kernel):
    ch, n = emb_cols.shape
    vmem = pl.BlockSpec(memory_space=pltpu.VMEM)
    return pl.pallas_call(
        pack_kernel,
        out_shape=(
            jax.ShapeDtypeStruct((2 * ch + 16, n), jnp.bfloat16),
            jax.ShapeDtypeStruct((4, ch, 9 * ch), jnp.bfloat16),
        ),
        in_specs=[vmem] * 6,
        out_specs=(vmem, vmem),
        compiler_params=pltpu.CompilerParams(vmem_limit_bytes=65472 * 1024),
        name="pack",
    )(
        emb_cols, emb_rows, valid.reshape(1, n), dil.reshape(1, 1), band.reshape(1, 1), kernel
    )


def tile_kernel(
    gathered, weights, cot_hbm,
    kept, sent, act_hbm, held_hbm,
    act, held, grd, slope, halo, edge, gedge, dfix, cols, colv, accs, kacc, kedge,
    place, nears, cot, sems,
):
    cot_in = pltpu.make_async_copy(cot_hbm, cot, sems.at[0])
    cot_in.start()
    ch = cot.shape[0]
    n = cot.shape[1]
    sub = ch // 8
    blocks = gathered.shape[0]
    extra = MAXDIL
    ext = n + 2 * extra
    packs = ext
    xhalo = ext + SLOT
    r_id = lax.axis_index("row")
    k_id = lax.axis_index("diag")
    settings = gathered[r_id, 2 * ch + 8 : 2 * ch + 16, :].astype(jnp.float32)
    r, high, rest = [jnp.max(settings[j : j + 1, :]).astype(jnp.int32) for j in range(3)]
    width = (high << WORD_BITS) + rest - k_id * n
    low = -k_id * n
    f32, bf16 = jnp.float32, jnp.bfloat16
    lane8 = lax.broadcasted_iota(jnp.int32, (8, n), 1)
    lane16 = lax.broadcasted_iota(jnp.int32, (16, n), 1)

    def small(x):
        return x.astype(f32).astype(bf16)

    reach = {s: small(s * r) for s in (1, 2, -1, -2)}
    zero = jnp.array(0, bf16)

    def block_of(index, first, count):
        found = gathered[jnp.clip(index, 0, blocks - 1), first : first + count, :]
        inside = ((index >= 0) & (index < blocks)).astype(f32)
        return found.astype(f32) * inside

    for t in range(4):
        cols[t] = block_of(r_id + k_id + t - 1, 0, ch).reshape(sub, 8, n)
        colv[t] = block_of(r_id + k_id + t - 1, 2 * ch, 8)

    tall = ch + 16

    def row_values(index):
        return block_of(index, ch, tall)

    own = row_values(r_id)
    own16 = own.astype(bf16)
    sublane = lax.broadcasted_iota(jnp.int32, (16, n), 0)
    ones = [(sublane == u).astype(f32).astype(bf16) for u in range(16)]
    ones = jnp.concatenate(ones, axis=1)

    def spread16(rows):
        wide = jnp.dot(rows[:, :16], ones, preferred_element_type=f32)
        parts = [wide[:, u * n : (u + 1) * n] for u in range(16)]
        return [(x[:ch].reshape(sub, 8, n), x[ch : ch + 8]) for x in parts]

    def unit(slot, rows, rows_v, col, col_v, inside):
        v = jnp.where(inside, rows_v * col_v, 0.0)
        h = (rows + col) * v[None]
        a, g = gelu_and_slope(h)
        slope[slot] = g * v[None]
        return v, h, a.reshape(ch, n).astype(bf16)

    def pick(t):
        col, col_v = cols[3], colv[3]
        for b in (2, 1, 0):
            here = t == b - 1
            col = jnp.where(here[None], cols[b], col)
            col_v = jnp.where(here, colv[b], col_v)
        return col, col_v

    def half(x):
        return x.reshape(2, 16, n)

    def keep(x, mask):
        return jnp.where(mask[None], half(x), jnp.zeros((2, 16, n), bf16)).reshape(ch, n)

    def turns(x, back):
        ahead, behind = pltpu.roll(x, r, 1), pltpu.roll(x, n - r, 1)
        return (behind, x, ahead) if back else (ahead, x, behind)

    def store_turns(ref, at, x, back):
        for tb, y in enumerate(turns(x, back)):
            ref[at, tb * ch : (tb + 1) * ch, :] = y

    def pack_lanes(lanes, p):
        loose = p + SLOT * ((lanes - p + EDGE) >> 4)
        return loose & (n - 1), lanes - loose

    lane1 = lax.broadcasted_iota(jnp.int32, (8, n), 1)
    whole = lax.broadcasted_iota(jnp.int32, (n, n), 0)

    def packs_step(g, carry):
        for two in range(2):
            p0 = 4 * g + 2 * two
            rows_at = [pack_lanes(lane1, p0 + w)[0][:1] for w in range(2)]
            to_row = jnp.concatenate(
                [(whole == x).astype(f32).astype(bf16) for x in rows_at], axis=1
            )
            place[2 * g + two] = to_row
            found = jnp.dot(own16, to_row, preferred_element_type=f32)
            for w in range(2):
                p = p0 + w
                row, e = pack_lanes(lane8, p)
                d = jnp.where(e < 0, e, e + n)
                col, col_v = pick((row + d) >> 7)
                mine = found[:, w * n : (w + 1) * n]
                _, _, a = unit(
                    packs + p, mine[:ch].reshape(sub, 8, n), mine[ch : ch + 8], col, col_v,
                    (d >= low) & (d < width),
                )
                halo[p] = a
        return carry

    lax.fori_loop(0, SLOT // 4, packs_step, 0)

    for at in list(range(2 * extra)) + list(range(n + 2 * extra, n + 4 * extra)):
        grd[at] = jnp.zeros(grd.shape[1:], bf16)

    def rows_step(g, carry):
        base = pl.multiple_of(g * 16, 16)
        turned = pltpu.roll(own, (n - base) & (n - 1), 1).astype(bf16)
        for u, (rows, rows_v) in enumerate(spread16(turned)):
            i = base + u
            here = lane8 >= i
            col = jnp.where(here[None], cols[1], cols[2])
            col_v = jnp.where(here, colv[1], colv[2])
            d = (lane8 - i) & (n - 1)
            v, h, a = unit(i + extra, rows, rows_v, col, col_v, (d >= low) & (d < width))
            held[i, :ch, :] = h.reshape(ch, n)
            held[i, ch:, :] = v
            store_turns(act, i + extra, a, False)
        return carry

    lax.fori_loop(0, n // 16, rows_step, 0)

    def grads_step(g, carry):
        base = pl.multiple_of(g * 16, 16)
        block = jnp.swapaxes(cot[:, pl.ds(base, 16), :], 0, 1)
        for u in range(16):
            i = base + u
            v = held[i, ch:, :]
            v2 = jnp.concatenate([v, v], axis=0).astype(bf16)
            x = (half(pltpu.roll(block[u], i, 1)) * v2[None]).reshape(ch, n)
            store_turns(grd, i + 2 * extra, x, True)
        return carry

    held_out = pltpu.make_async_copy(
        held.at[pl.ds(0, n)], held_hbm.at[pl.ds(0, n)], sems.at[2]
    )
    held_out.start()
    cot_in.wait()
    lax.fori_loop(0, n // 16, grads_step, 0)

    def edges_step(p, carry):
        row = small(pack_lanes(lane16, p)[0])
        a = x = jnp.zeros((2, 16, n), bf16)
        for m in range(n // SLOT):
            i = p + m * SLOT
            here = (row == small(i))[None]
            a = jnp.where(here, half(act[i + extra, ch : 2 * ch, :]), a)
            x = jnp.where(here, half(grd[i + 2 * extra, ch : 2 * ch, :]), x)
        edge[p] = a.reshape(ch, n)
        gedge[p] = x.reshape(ch, n)
        return carry

    lax.fori_loop(0, SLOT, edges_step, 0)

    lane_tall = lax.broadcasted_iota(jnp.int32, (tall, n), 1)
    near = jnp.where(
        lane_tall < extra,
        pltpu.roll(row_values(r_id - 1), extra, 1),
        pltpu.roll(row_values(r_id + 1), extra, 1),
    )
    for y, (rows, rows_v) in enumerate(spread16(near.astype(bf16))[: 2 * extra]):
        nears[y, :sub] = rows
        nears[y, sub] = rows_v

    def near_row(y):
        return jnp.where(y < extra, y - extra, n + y - extra)

    def near_lanes(i):
        e = ((lane8 - i + EDGE) & (n - 1)) - EDGE
        return e, jnp.where(e < 0, e, e + n)

    def near_step(g, carry):
        for w in range(4):
            y = 4 * g + w
            i = near_row(y)
            rows, rows_v = nears[y, :sub], nears[y, sub]
            e, d = near_lanes(i)
            col, col_v = pick((i + d) >> 7)
            inside = (e < EDGE) & (d >= low) & (d < width)
            _, _, far = unit(xhalo + y, rows, rows_v, col, col_v, inside)
            d = (lane8 - i) & (n - 1)
            col, col_v = pick((i + d) >> 7)
            _, _, a = unit(i + extra, rows, rows_v, col, col_v, (d >= low) & (d < width))
            store_turns(act, i + extra, a, False)
            slot = (small((lane16 - i + EDGE) & (n - 1)) < jnp.array(SLOT, bf16))[None]
            q = i & (SLOT - 1)
            halo[SLOT + y] = jnp.where(slot, half(far), half(halo[q])).reshape(ch, n)
            edge[SLOT + y] = jnp.where(slot, half(a), half(edge[q])).reshape(ch, n)
        return carry

    lax.fori_loop(0, extra // 2, near_step, 0)
    act_out = pltpu.make_async_copy(act, act_hbm, sems.at[3])
    act_out.start()

    w_in = weights[1]
    w_out_edge, w_in_edge = weights[2, :, : 6 * ch], weights[3, :, : 6 * ch]
    crossing = crossings()
    kedge[...] = jnp.zeros(kedge.shape, f32)
    rows_last = small(n - r)

    def fix_taps(p):
        row, e = pack_lanes(lane16, p)
        row, e = small(row), small(e)
        found, wrong, away = [], [], []
        for ta in range(3):
            q = (p + (ta - 1) * r) & (SLOT - 1)
            at = q
            if ta == 0:
                at = jnp.where(p < r, q + extra, q)
            elif ta == 2:
                at = jnp.where(p + r >= SLOT, q + SLOT + extra, q)
            far, own_edge = turns(halo[at], False), turns(edge[at], False)
            back = turns(gedge[(p - (ta - 1) * r) & (SLOT - 1)], True)
            for tb in range(3):
                s = tb - ta
                if s == 0:
                    continue
                if s > 0:
                    mask = (e >= reach[-s]) & (e < zero)
                    spill = (e >= zero) & (e < reach[s])
                else:
                    mask = (e >= zero) & (e < reach[-s])
                    spill = (e >= reach[s]) & (e < zero)
                if ta == 0:
                    spill = spill & (row < rows_last)
                elif ta == 2:
                    spill = spill & (row >= reach[1])
                found.append(keep(far[tb], mask))
                wrong.append(keep(own_edge[tb], mask))
                away.append(keep(back[tb], spill))
        return [jnp.concatenate(x, axis=0) for x in (found, wrong, away)]

    def fix_pair(p):
        found, wrong, away = [
            jnp.concatenate(x, axis=1) for x in zip(fix_taps(p), fix_taps(p + 1))
        ]
        grads = jnp.concatenate([gedge[p], gedge[p + 1]], axis=1)
        z = jnp.dot(w_out_edge, found, preferred_element_type=f32) - jnp.dot(
            w_out_edge, wrong, preferred_element_type=f32
        )
        lanes = (((1,), (1,)), ((), ()))
        kedge[...] += lax.dot_general(
            found, grads, lanes, preferred_element_type=f32
        ) - lax.dot_general(wrong, grads, lanes, preferred_element_type=f32)
        da = jnp.dot(w_in_edge, away, preferred_element_type=f32)
        for w in range(2):
            held[n + p + w, :ch, :] = z[:, w * n : (w + 1) * n]
            dfix[p + w] = da[:, w * n : (w + 1) * n].reshape(sub, 8, n)

    def fix_step(g, carry):
        fix_pair(4 * g)
        fix_pair(4 * g + 2)
        return carry

    lax.fori_loop(0, SLOT // 4, fix_step, 0)
    fixes_out = pltpu.make_async_copy(
        held.at[pl.ds(n, SLOT)], held_hbm.at[pl.ds(n, SLOT)], sems.at[4]
    )
    fixes_out.start()

    for y in range(2 * extra):
        i = y - extra if y < extra else n + y - extra
        ta = 0 if y < extra else 2
        e = small(((lane16 - i + EDGE) & (n - 1)) - EDGE)
        parts = []
        for tb in range(3):
            s = tb - ta
            x = grd[i + (1 - ta) * r + 2 * extra, tb * ch : (tb + 1) * ch, :]
            if s > 0:
                parts.append(keep(x, (e >= zero) & (e < reach[s])))
            elif s < 0:
                parts.append(keep(x, (e >= reach[s]) & (e < zero)))
        first = 1 if ta == 0 else 6
        weights = w_in[:, first * ch : (first + 2) * ch]
        da = jnp.dot(weights, jnp.concatenate(parts, axis=0), preferred_element_type=f32)
        dfix[SLOT + y] = da.reshape(sub, 8, n)

    kacc[...] = jnp.zeros(kacc.shape, f32)
    accs[...] = jnp.zeros(accs.shape, f32)
    def spreads(i):
        both = two_rows(grd, i + 2 * extra, -r)
        da = jnp.dot(w_in, both, preferred_element_type=f32)
        return [da[:, w * n : (w + 1) * n].reshape(sub, 8, n) for w in range(2)]

    def kernel_part(i):
        both = jnp.concatenate([act[i + extra], act[i + extra + 1]], axis=1)
        grads = [
            jnp.concatenate(
                [grd[i + w + t * r + 2 * extra, ch : 2 * ch, :] for t in (1, 0, -1)], axis=0
            )
            for w in range(2)
        ]
        return lax.dot_general(
            both, jnp.concatenate(grads, axis=1), (((1,), (1,)), ((), ())),
            preferred_element_type=f32,
        )

    def back_step(g, carry):
        base = pl.multiple_of(g * 16, 16)
        total = None
        racc, c0, c1, bacc = accs[1], accs[4], accs[5], accs[7]
        for u in range(0, 16, 2):
            i = base + u
            part = kernel_part(i)
            total = part if total is None else total + part
            for w, da in enumerate(spreads(i)):
                slot = ((lane8 - (i + w) + EDGE) & (n - 1)) < SLOT
                da = da - jnp.where(slot[None], dfix[u + w], 0.0)
                gg = grd[i + w + 2 * extra, ch : 2 * ch, :].astype(f32).reshape(sub, 8, n)
                bacc = bacc + gg
                dx = gg + slope[i + w + extra] * da
                racc = racc + jnp.where(
                    (lane8 == i + w)[None], jnp.sum(dx, axis=2, keepdims=True), 0.0
                )
                here = (lane8 >= i + w)[None]
                c0 = c0 + jnp.where(here, dx, 0.0)
                c1 = c1 + jnp.where(here, 0.0, dx)
        accs[1], accs[4], accs[5], accs[7] = racc, c0, c1, bacc
        kacc[...] += total
        return carry

    lax.fori_loop(0, n // 16, back_step, 0)

    def add_columns(dx, t):
        for b in range(4):
            accs[3 + b] += jnp.where((t == b - 1)[None], dx, 0.0)

    def near_sums(g, carry):
        y0 = 2 * g
        i0 = near_row(y0)
        which = jnp.where(y0 < extra, 0, 2)
        for w, da in enumerate(spreads(i0)):
            i = i0 + w
            e, d = near_lanes(i)
            fix = dfix[SLOT + y0 + w]
            inner = slope[i + extra] * (da - fix)
            outer = slope[xhalo + y0 + w] * fix
            add_columns(inner, (i + ((lane8 - i) & (n - 1))) >> 7)
            add_columns(outer, (i + d) >> 7)
            total = jnp.sum(inner + outer, axis=2, keepdims=True)
            accs[which] += jnp.where((lane8 == (i & (n - 1)))[None], total, 0.0)
        kacc[...] += kernel_part(i0)
        return carry

    lax.fori_loop(0, extra, near_sums, 0)

    def pack_sums(g, carry):
        for two in range(2):
            dxs = []
            for w in range(2):
                p = 4 * g + 2 * two + w
                row, e = pack_lanes(lane8, p)
                dx = slope[packs + p] * dfix[p]
                add_columns(dx, (row + jnp.where(e < 0, e, e + n)) >> 7)
                dxs.append(dx.reshape(ch, n))
            rest = jnp.concatenate(dxs, axis=1)
            parts = []
            for _ in range(3):
                part = rest.astype(bf16)
                rest = rest - part.astype(f32)
                parts.append(part)
            found = lax.dot_general(
                jnp.concatenate(parts, axis=0), place[2 * g + two],
                (((1,), (1,)), ((), ())), preferred_element_type=f32,
            )
            total = found[:ch] + found[ch : 2 * ch] + found[2 * ch :]
            accs[1] += total.reshape(sub, 8, n)
        return carry

    lax.fori_loop(0, SLOT // 4, pack_sums, 0)

    half_blocks = blocks // 2
    mine = r_id // half_blocks
    kept[...] = jnp.zeros(kept.shape, f32)
    sent[...] = jnp.zeros(sent.shape, f32)

    def put(at, first, value):
        which = jnp.where(at >= half_blocks, 1, 0)
        slot = pl.multiple_of((at - which * half_blocks) * 2 * ch + first, ch)

        @pl.when((at >= 0) & (at < blocks) & (which == mine))
        def _():
            kept[pl.ds(slot, ch), :] = value

        @pl.when((at >= 0) & (at < blocks) & (which != mine))
        def _():
            sent[pl.ds(slot, ch), :] = value

    for t in range(3):
        put(r_id + t - 1, 0, accs[t].reshape(ch, n))
    for t in range(4):
        put(r_id + k_id + t - 1, ch, accs[3 + t].reshape(ch, n))

    parts = []
    for ta in range(3):
        part = kacc[:, ta * ch : (ta + 1) * ch]
        fixes = [
            kedge[crossing.index((ta, tb)) * ch : (crossing.index((ta, tb)) + 1) * ch, :]
            if ta != tb
            else jnp.zeros((ch, ch), f32)
            for tb in range(3)
        ]
        parts.append(part + jnp.concatenate(fixes, axis=0))
    full = jnp.concatenate(parts, axis=0).T
    full = jnp.concatenate([full, jnp.zeros((ch, 3 * n - 9 * ch), f32)], axis=1)
    lanes = lax.broadcasted_iota(jnp.int32, (ch, 3 * n), 1)
    btotal = jnp.sum(accs[7].reshape(ch, n), axis=1, keepdims=True)
    full = jnp.where(lanes == 9 * ch, btotal, full)
    for t in range(3):
        first = half_blocks * 2 * ch + t * ch
        sent[first : first + ch, :] = full[:, t * n : (t + 1) * n]
    held_out.wait()
    act_out.wait()
    fixes_out.wait()


def rows_of(ref, at, step):
    return jnp.concatenate([ref[at - step], ref[at], ref[at + step]], axis=0)


def two_rows(ref, at, step):
    return jnp.concatenate([rows_of(ref, at, step), rows_of(ref, at + 1, step)], axis=1)


def out_kernel(
    start, count, weights_hbm, bias_hbm, dil_hbm, act_hbm, held_hbm, *refs
):
    pair_out, weights, bias, act, held, done, dil, sems, act_sems, held_sems, done_sems = refs[-11:]
    f32, bf16 = jnp.float32, jnp.bfloat16
    ch, n = pair_out.shape[:2]
    sub = ch // 8

    def part(hbm, vmem, sem, first, there):
        rows = pl.ds(pl.multiple_of(first, 16), 16)
        return pltpu.make_async_copy(hbm.at[rows], vmem.at[pl.ds(there, 16)], sem)

    def act_part(g):
        return part(act_hbm, act, act_sems.at[g], (start + g) * 16, g * 16)

    def held_part(g):
        return part(held_hbm, held, held_sems.at[g], (start + g) * 16, g * 16)

    def done_part(g):
        rows = pl.ds(pl.multiple_of((start + g) * 16, 16), 16)
        return pltpu.make_async_copy(done.at[g], pair_out.at[:, rows, :], done_sems.at[g])

    fixes = part(held_hbm, held, held_sems.at[count], n, count * 16)
    small = [
        pltpu.make_async_copy(a, b, sems.at[j])
        for j, (a, b) in enumerate(
            ((dil_hbm, dil), (bias_hbm, bias), (weights_hbm.at[0], weights))
        )
    ]
    for copy in small:
        copy.start()
    fixes.start()
    act_part(0).start()
    for g in range(count):
        act_part(g + 1).start()
        held_part(g).start()
    lane8 = lax.broadcasted_iota(jnp.int32, (8, n), 1)
    for copy in small:
        copy.wait()
    w_out = weights[...]
    square = [lax.broadcasted_iota(jnp.int32, (ch, ch), x) for x in range(2)]
    shift_by = jnp.sum(
        jnp.where(square[0] == square[1], jnp.broadcast_to(bias[...], (ch, ch)), 0.0),
        axis=1, keepdims=True,
    )
    shift_by = jnp.broadcast_to(shift_by, (ch, n)).reshape(sub, 8, n)
    r = jnp.max(dil[...])
    fixes.wait()
    act_part(0).wait()

    def conv_step(g, carry):
        act_part(g + 1).wait()
        held_part(g).wait()
        found = []
        for u in range(0, 16, 2):
            k = g * 16 + u
            i = start * 16 + k
            z = jnp.dot(w_out, two_rows(act, k + MAXDIL, r), preferred_element_type=f32)
            for w in range(2):
                slot = ((lane8 - (i + w) + EDGE) & (n - 1)) < SLOT
                fix = held[count * 16 + u + w, :ch, :].reshape(sub, 8, n)
                y = (held[k + w, :ch, :] + z[:, w * n : (w + 1) * n]).reshape(sub, 8, n)
                y = y + shift_by + jnp.where(slot[None], fix, 0.0)
                y = (y * held[k + w, ch:, :][None]).reshape(ch, n).astype(bf16)
                found.append(pltpu.roll(y, (n - i - w) & (n - 1), 1))
        done[g] = jnp.swapaxes(jnp.stack(found), 0, 1)
        done_part(g).start()
        return carry

    lax.fori_loop(0, count, conv_step, 0)
    for g in range(count):
        done_part(g).wait()


def out_call(start, count, made, weights, bias, dil, act, held):
    _, ch3, n = act.shape
    ch = ch3 // 3
    hbm = pl.BlockSpec(memory_space=pltpu.HBM)
    dma = pltpu.SemaphoreType.DMA

    def body(*refs):
        out_kernel(start, count, *refs)

    return pl.pallas_call(
        body,
        out_shape=jax.ShapeDtypeStruct((ch, n, n), jnp.bfloat16),
        in_specs=[hbm] * (5 + len(made)),
        out_specs=hbm,
        input_output_aliases={5: 0} if made else {},
        scratch_shapes=[
            pltpu.VMEM(weights.shape[1:], weights.dtype),
            pltpu.VMEM((1, ch), jnp.float32),
            pltpu.VMEM((16 * (count + 1), ch3, n), act.dtype),
            pltpu.VMEM((16 * (count + 1), ch + 8, n), held.dtype),
            pltpu.VMEM((count, ch, 16, n), jnp.bfloat16),
            pltpu.VMEM((1, 1), jnp.int32),
            dma((3,)),
            dma((count + 1,)),
            dma((count + 1,)),
            dma((count,)),
        ],
        compiler_params=pltpu.CompilerParams(vmem_limit_bytes=OUT_LIMIT),
        cost_estimate=pl.CostEstimate(
            flops=288 * count * ch * ch * n, bytes_accessed=200 * count * ch * n, transcendentals=0
        ),
        name="outputs",
    )(weights, bias.reshape(1, ch), dil.reshape(1, 1), act, held, *made)


def tile_call(gathered, weights, cot):
    blocks, _, n = gathered.shape
    ch = cot.shape[0]
    assert blocks % 2 == 0
    sub = ch // 8
    f32, bf16 = jnp.float32, jnp.bfloat16
    vmem = pl.BlockSpec(memory_space=pltpu.VMEM)
    hbm = pl.BlockSpec(memory_space=pltpu.HBM)
    near = 2 * MAXDIL
    units = n + 2 * near + SLOT
    return pl.pallas_call(
        tile_kernel,
        out_shape=(
            jax.ShapeDtypeStruct((blocks * ch, n), f32),
            jax.ShapeDtypeStruct((blocks * ch + 3 * ch, n), f32),
            jax.ShapeDtypeStruct((n + SLOT, 3 * ch, n), bf16),
            jax.ShapeDtypeStruct((n + SLOT, ch + 8, n), f32),
        ),
        in_specs=[vmem, vmem, hbm],
        out_specs=(vmem, vmem, hbm, hbm),
        scratch_shapes=[
            pltpu.VMEM((n + SLOT, 3 * ch, n), bf16),
            pltpu.VMEM((n + SLOT, ch + 8, n), f32),
            pltpu.VMEM((n + 2 * near, 3 * ch, n), bf16),
            pltpu.VMEM((units, sub, 8, n), f32),
            pltpu.VMEM((SLOT + near, ch, n), bf16),
            pltpu.VMEM((SLOT + near, ch, n), bf16),
            pltpu.VMEM((SLOT, ch, n), bf16),
            pltpu.VMEM((SLOT + near, sub, 8, n), f32),
            pltpu.VMEM((4, sub, 8, n), f32),
            pltpu.VMEM((4, 8, n), f32),
            pltpu.VMEM((8, sub, 8, n), f32),
            pltpu.VMEM((3 * ch, 3 * ch), f32),
            pltpu.VMEM((6 * ch, ch), f32),
            pltpu.VMEM((SLOT // 2, n, 2 * n), bf16),
            pltpu.VMEM((near, sub + 1, 8, n), f32),
            pltpu.VMEM((ch, n, n), bf16),
            pltpu.SemaphoreType.DMA((5,)),
        ],
        compiler_params=pltpu.CompilerParams(vmem_limit_bytes=VMEM_LIMIT),
        cost_estimate=pl.CostEstimate(
            flops=54 * ch * ch * n * n, bytes_accessed=16 * ch * n * n, transcendentals=ch * n * n
        ),
        name="tile",
    )(gathered, weights, cot)


def final_kernel(scales, x, y, rows, cols, kgrad, bgrad):
    ch = rows.shape[0]
    n = rows.shape[1]
    total = x[...] + y[...]
    rows[...] = total[:ch] * scales[0]
    cols[...] = total[ch : 2 * ch] * scales[0]
    total = total[2 * ch :] * scales[1]
    for t in range(9):
        first, lane = (t * ch // n) * ch, t * ch % n
        kgrad[t] = total[first : first + ch, lane : lane + ch]
    first, lane = (9 * ch // n) * ch, 9 * ch % n
    part = jnp.broadcast_to(total[first : first + ch, lane : lane + 1], (ch, ch))
    square = [lax.broadcasted_iota(jnp.int32, (ch, ch), i) for i in range(2)]
    bgrad[...] = jnp.sum(jnp.where(square[0] == square[1], part, 0.0), axis=0, keepdims=True)


def final_call(x, y, embed_scale, weight_scale):
    n = x.shape[1]
    ch = x.shape[0] // 5
    f32 = jnp.float32

    def body(*refs):
        final_kernel((embed_scale, weight_scale), *refs)

    vmem = pl.BlockSpec(memory_space=pltpu.VMEM)
    return pl.pallas_call(
        body,
        out_shape=(
            jax.ShapeDtypeStruct((ch, n), f32),
            jax.ShapeDtypeStruct((ch, n), f32),
            jax.ShapeDtypeStruct((9, ch, ch), f32),
            jax.ShapeDtypeStruct((1, ch), f32),
        ),
        in_specs=[vmem, vmem],
        out_specs=(vmem,) * 4,
        compiler_params=pltpu.CompilerParams(vmem_limit_bytes=2 * 1024 * 1024),
        name="finish",
    )(x, y)


def swapped(value, axis, bit):
    return lax.ppermute(value, axis, [(i, i ^ bit) for i in range(lax.axis_size(axis))])


def local(emb_rows, emb_cols, kernel, bias, cotangent, valid, dilation, band):
    ch, n = emb_rows.shape
    row_devices, diag_devices = lax.axis_size("row"), lax.axis_size("diag")
    assert cotangent.shape[2] == n == 128
    assert row_devices & (row_devices - 1) == 0 and diag_devices & (diag_devices - 1) == 0
    total_diags = n * diag_devices
    bins, weights = pack_call(emb_cols, emb_rows, valid, dilation, band, kernel)
    gathered = lax.all_gather(bins, "row")
    kept, sent, *held = tile_call(gathered, weights, cotangent)
    groups = n // 16
    cut = groups - groups * 3 // 8
    made = ()

    place = lax.axis_index("row")
    bit = row_devices // 2
    while True:
        came = swapped(sent, "row", bit)
        if not made:
            made = (out_call(0, cut, (), weights, bias, dilation, *held),)
            came, *made = lax.optimization_barrier((came, *made))
        own = bit * 2 * ch
        sums, whole = kept + came[:own], sent[own:] + came[own:]
        bit //= 2
        if not bit:
            break
        halves = sums.reshape(2, bit * 2 * ch, n)
        mine = (place // bit) & 1
        kept = lax.dynamic_index_in_dim(halves, mine, 0, False)
        other = lax.dynamic_index_in_dim(halves, 1 - mine, 0, False)
        sent = jnp.concatenate([other, whole], axis=0)
    both = jnp.concatenate([sums, whole], axis=0)
    bit = 1
    while 2 * bit < diag_devices:
        both = both + swapped(both, "diag", bit)
        bit *= 2
    came = swapped(both, "diag", bit)
    pair_out = out_call(cut, groups - cut, tuple(made), weights, bias, dilation, *held)
    came, pair_out = lax.optimization_barrier((came, pair_out))
    rows, cols, kgrad, bgrad = final_call(
        both,
        came,
        1.0 / total_diags**0.5,
        1.0 / (row_devices * n * total_diags) ** 0.5,
    )
    return pair_out, rows, cols, kgrad.reshape(3, 3, ch, ch), bgrad.reshape(ch)


def solution(mesh):
    in_specs = (
        P(None, ("grp", "row")),
        P(None, ("grp", "row")),
        P(),
        P(),
        P(None, ("grp", "row"), "diag"),
        P(("grp", "row")),
        P("grp"),
        P("grp"),
    )
    out_specs = (
        P(None, ("grp", "row"), "diag"),
        P(None, ("grp", "row")),
        P(None, ("grp", "row")),
        P("grp", None, None, None),
        P("grp"),
    )
    return jax.shard_map(local, mesh=mesh, in_specs=in_specs, out_specs=out_specs, check_vma=False)
```

```python
import jax
import jax.numpy as jnp
from jax import lax
from jax.experimental import pallas as pl
from jax.experimental.pallas import tpu as pltpu
from jax.sharding import PartitionSpec as P

MAXDIL = 4
BACK = 64
EDGE = 2 * MAXDIL
SLOT = 2 * EDGE
GELU_C = 0.7978845608028654
GELU_A = 0.044715
WORD_BITS = 6
VMEM_LIMIT = 54600 * 1024
OUT_LIMIT = (65472 - 1500) * 1024


def gelu_and_slope(h):
    square = h * h
    t = jnp.tanh(h * (GELU_C + (GELU_C * GELU_A) * square))
    half = 0.5 * h
    one = 1.0 + t
    slope = 0.5 * one + half * (1.0 - t * t) * (GELU_C + (3.0 * GELU_C * GELU_A) * square)
    return half * one, slope


def crossings():
    return [(ta, tb) for ta in range(3) for tb in range(3) if ta != tb]


def pack_kernel(emb_cols, emb_rows, valid, dil, band, kernel, bins, weights):
    f32, bf16 = jnp.float32, jnp.bfloat16
    ch, n = emb_cols.shape
    bins[:ch] = emb_cols[...]
    bins[ch : 2 * ch] = emb_rows[...]
    known = jnp.broadcast_to(valid[...].astype(f32), (8, n))
    wide = jnp.broadcast_to(band[...], (8, n))
    line = lax.broadcasted_iota(jnp.int32, (8, n), 0)
    settings = jnp.where(line == 1, wide >> WORD_BITS, wide & (2**WORD_BITS - 1))
    settings = jnp.where(line == 0, jnp.broadcast_to(dil[...], (8, n)), settings)
    bins[2 * ch :] = jnp.concatenate([known, settings.astype(f32)], axis=0).astype(bf16)
    taps = [kernel[t // 3, t % 3] for t in range(9)]
    turned = [w.astype(f32).T.astype(bf16) for w in taps]
    cross = [3 * ta + tb for ta, tb in crossings()]
    weights[0] = jnp.concatenate(taps, axis=1)
    weights[1] = jnp.concatenate(turned, axis=1)
    weights[2, :, : 6 * ch] = jnp.concatenate([taps[t] for t in cross], axis=1)
    weights[3, :, : 6 * ch] = jnp.concatenate([turned[t] for t in cross], axis=1)


def pack_call(emb_cols, emb_rows, valid, dil, band, kernel):
    ch, n = emb_cols.shape
    vmem = pl.BlockSpec(memory_space=pltpu.VMEM)
    return pl.pallas_call(
        pack_kernel,
        out_shape=(
            jax.ShapeDtypeStruct((2 * ch + 16, n), jnp.bfloat16),
            jax.ShapeDtypeStruct((16, ch, 9 * ch), jnp.bfloat16),
        ),
        in_specs=[vmem] * 6,
        out_specs=(vmem, vmem),
        compiler_params=pltpu.CompilerParams(vmem_limit_bytes=65472 * 1024),
        name="pack",
    )(
        emb_cols, emb_rows, valid.reshape(1, n), dil.reshape(1, 1), band.reshape(1, 1), kernel
    )


def tile_kernel(
    gathered, weights_hbm, cot_hbm,
    kept, sent, act_hbm, held_hbm,
    act, held, grd, slope, halo, edge, gedge, dfix, cols, colv, accs, kacc, kedge,
    place, nears, spreads, cot, weights, sems,
):
    cot_in = pltpu.make_async_copy(cot_hbm, cot, sems.at[0])
    cot_in.start()
    weights_in = pltpu.make_async_copy(weights_hbm.at[pl.ds(0, 4)], weights, sems.at[1])
    weights_in.start()
    ch = cot.shape[0]
    n = cot.shape[1]
    sub = ch // 8
    blocks = gathered.shape[0]
    extra = MAXDIL
    ext = n + 2 * extra
    packs = ext
    xhalo = ext + SLOT
    r_id = lax.axis_index("row")
    k_id = lax.axis_index("diag")
    settings = gathered[r_id, 2 * ch + 8 : 2 * ch + 16, :].astype(jnp.float32)
    r, high, rest = [jnp.max(settings[j : j + 1, :]).astype(jnp.int32) for j in range(3)]
    width = (high << WORD_BITS) + rest - k_id * n
    low = -k_id * n
    f32, bf16 = jnp.float32, jnp.bfloat16
    lane8 = lax.broadcasted_iota(jnp.int32, (8, n), 1)
    lane16 = lax.broadcasted_iota(jnp.int32, (16, n), 1)

    def small(x):
        return x.astype(f32).astype(bf16)

    reach = {s: small(s * r) for s in (1, 2, -1, -2)}
    zero = jnp.array(0, bf16)

    def block_of(index, first, count):
        found = gathered[jnp.clip(index, 0, blocks - 1), first : first + count, :]
        inside = ((index >= 0) & (index < blocks)).astype(f32)
        return found.astype(f32) * inside

    for t in range(4):
        cols[t] = block_of(r_id + k_id + t - 1, 0, ch).reshape(sub, 8, n)
        colv[t] = block_of(r_id + k_id + t - 1, 2 * ch, 8)

    tall = ch + 16

    def row_values(index):
        return block_of(index, ch, tall)

    own = row_values(r_id)
    own16 = own.astype(bf16)
    sublane = lax.broadcasted_iota(jnp.int32, (16, n), 0)
    ones = [(sublane == u).astype(f32).astype(bf16) for u in range(16)]
    ones = jnp.concatenate(ones, axis=1)

    def spread16(rows):
        wide = jnp.dot(rows[:, :16], ones, preferred_element_type=f32)
        parts = [wide[:, u * n : (u + 1) * n] for u in range(16)]
        return [(x[:ch].reshape(sub, 8, n), x[ch : ch + 8]) for x in parts]

    def unit(slot, rows, rows_v, col, col_v, inside):
        v = jnp.where(inside, rows_v * col_v, 0.0)
        h = (rows + col) * v[None]
        a, g = gelu_and_slope(h)
        slope[slot] = g * v[None]
        return v, h, a.reshape(ch, n).astype(bf16)

    def pick(t):
        col, col_v = cols[3], colv[3]
        for b in (2, 1, 0):
            here = t == b - 1
            col = jnp.where(here[None], cols[b], col)
            col_v = jnp.where(here, colv[b], col_v)
        return col, col_v

    def half(x):
        return x.reshape(2, 16, n)

    def keep(x, mask):
        return jnp.where(mask[None], half(x), jnp.zeros((2, 16, n), bf16)).reshape(ch, n)

    def turns(x, back):
        ahead, behind = pltpu.roll(x, r, 1), pltpu.roll(x, n - r, 1)
        return (behind, x, ahead) if back else (ahead, x, behind)

    def store_turns(ref, at, x, back):
        for tb, y in enumerate(turns(x, back)):
            ref[at, tb * ch : (tb + 1) * ch, :] = y

    def pack_lanes(lanes, p):
        loose = p + SLOT * ((lanes - p + EDGE) >> 4)
        return loose & (n - 1), lanes - loose

    lane1 = lax.broadcasted_iota(jnp.int32, (8, n), 1)
    whole = lax.broadcasted_iota(jnp.int32, (n, n), 0)

    def packs_step(g, carry):
        for two in range(4):
            p0 = 8 * g + 2 * two
            rows_at = [pack_lanes(lane1, p0 + w)[0][:1] for w in range(2)]
            to_row = jnp.concatenate(
                [(whole == x).astype(f32).astype(bf16) for x in rows_at], axis=1
            )
            place[4 * g + two] = to_row
            found = jnp.dot(own16, to_row, preferred_element_type=f32)
            for w in range(2):
                p = p0 + w
                row, e = pack_lanes(lane8, p)
                d = jnp.where(e < 0, e, e + n)
                col, col_v = pick((row + d) >> 7)
                mine = found[:, w * n : (w + 1) * n]
                _, _, a = unit(
                    packs + p, mine[:ch].reshape(sub, 8, n), mine[ch : ch + 8], col, col_v,
                    (d >= low) & (d < width),
                )
                halo[p] = a
        return carry

    lax.fori_loop(0, SLOT // 8, packs_step, 0)

    for at in list(range(2 * extra)) + list(range(n + 2 * extra, n + 4 * extra)):
        grd[at] = jnp.zeros(grd.shape[1:], bf16)

    for g in range(n // 16):
        turned = pltpu.roll(own, (n - 16 * g) % n, 1).astype(bf16) if g else own16
        wide = jnp.dot(turned[:, :16], ones, preferred_element_type=f32)
        for u in range(16):
            spreads[16 * g + u] = wide[: ch + 8, u * n : (u + 1) * n]

    def rows_step(g, carry):
        base = pl.multiple_of(g * 32, 32)
        for u in range(32):
            i = base + u
            rows, rows_v = spreads[i, :ch, :].reshape(sub, 8, n), spreads[i, ch:, :]
            here = lane8 >= i
            col = jnp.where(here[None], cols[1], cols[2])
            col_v = jnp.where(here, colv[1], colv[2])
            d = (lane8 - i) & (n - 1)
            v, h, a = unit(i + extra, rows, rows_v, col, col_v, (d >= low) & (d < width))
            held[i, :ch, :] = h.reshape(ch, n)
            held[i, ch:, :] = v
            store_turns(act, i + extra, a, False)
        return carry

    lax.fori_loop(0, n // 32, rows_step, 0)

    def grads_step(g, carry):
        base = pl.multiple_of(g * 16, 16)
        block = jnp.swapaxes(cot[:, pl.ds(base, 16), :], 0, 1)
        for u in range(16):
            i = base + u
            v = held[i, ch:, :]
            v2 = jnp.concatenate([v, v], axis=0).astype(bf16)
            x = (half(pltpu.roll(block[u], i, 1)) * v2[None]).reshape(ch, n)
            store_turns(grd, i + 2 * extra, x, True)
        return carry

    held_out = pltpu.make_async_copy(
        held.at[pl.ds(0, n)], held_hbm.at[pl.ds(0, n)], sems.at[2]
    )
    held_out.start()
    cot_in.wait()
    lax.fori_loop(0, n // 16, grads_step, 0)

    def edges_step(g, carry):
        for w in range(4):
            p = 4 * g + w
            row = small(pack_lanes(lane16, p)[0])
            a = x = jnp.zeros((2, 16, n), bf16)
            for m in range(n // SLOT):
                i = p + m * SLOT
                here = (row == small(i))[None]
                a = jnp.where(here, half(act[i + extra, ch : 2 * ch, :]), a)
                x = jnp.where(here, half(grd[i + 2 * extra, ch : 2 * ch, :]), x)
            edge[p] = a.reshape(ch, n)
            gedge[p] = x.reshape(ch, n)
        return carry

    lax.fori_loop(0, SLOT // 4, edges_step, 0)

    lane_tall = lax.broadcasted_iota(jnp.int32, (tall, n), 1)
    near = jnp.where(
        lane_tall < extra,
        pltpu.roll(row_values(r_id - 1), extra, 1),
        pltpu.roll(row_values(r_id + 1), extra, 1),
    )
    for y, (rows, rows_v) in enumerate(spread16(near.astype(bf16))[: 2 * extra]):
        nears[y, :sub] = rows
        nears[y, sub] = rows_v

    def near_row(y):
        return jnp.where(y < extra, y - extra, n + y - extra)

    def near_lanes(i):
        e = ((lane8 - i + EDGE) & (n - 1)) - EDGE
        return e, jnp.where(e < 0, e, e + n)

    def near_step(g, carry):
        for w in range(4):
            y = 4 * g + w
            i = near_row(y)
            rows, rows_v = nears[y, :sub], nears[y, sub]
            e, d = near_lanes(i)
            col, col_v = pick((i + d) >> 7)
            inside = (e < EDGE) & (d >= low) & (d < width)
            _, _, far = unit(xhalo + y, rows, rows_v, col, col_v, inside)
            d = (lane8 - i) & (n - 1)
            col, col_v = pick((i + d) >> 7)
            _, _, a = unit(i + extra, rows, rows_v, col, col_v, (d >= low) & (d < width))
            store_turns(act, i + extra, a, False)
            slot = (small((lane16 - i + EDGE) & (n - 1)) < jnp.array(SLOT, bf16))[None]
            q = i & (SLOT - 1)
            halo[SLOT + y] = jnp.where(slot, half(far), half(halo[q])).reshape(ch, n)
            edge[SLOT + y] = jnp.where(slot, half(a), half(edge[q])).reshape(ch, n)
        return carry

    lax.fori_loop(0, extra // 2, near_step, 0)
    act_out = pltpu.make_async_copy(act, act_hbm, sems.at[3])
    act_out.start()

    weights_in.wait()
    w_in = weights[1]
    w_out_edge, w_in_edge = weights[2, :, : 6 * ch], weights[3, :, : 6 * ch]
    crossing = crossings()
    kedge[...] = jnp.zeros(kedge.shape, f32)
    rows_last = small(n - r)

    def fix_taps(p):
        row, e = pack_lanes(lane16, p)
        row, e = small(row), small(e)
        found, wrong, away = [], [], []
        for ta in range(3):
            q = (p + (ta - 1) * r) & (SLOT - 1)
            at = q
            if ta == 0:
                at = jnp.where(p < r, q + extra, q)
            elif ta == 2:
                at = jnp.where(p + r >= SLOT, q + SLOT + extra, q)
            far, own_edge = turns(halo[at], False), turns(edge[at], False)
            back = turns(gedge[(p - (ta - 1) * r) & (SLOT - 1)], True)
            for tb in range(3):
                s = tb - ta
                if s == 0:
                    continue
                if s > 0:
                    mask = (e >= reach[-s]) & (e < zero)
                    spill = (e >= zero) & (e < reach[s])
                else:
                    mask = (e >= zero) & (e < reach[-s])
                    spill = (e >= reach[s]) & (e < zero)
                if ta == 0:
                    spill = spill & (row < rows_last)
                elif ta == 2:
                    spill = spill & (row >= reach[1])
                found.append(keep(far[tb], mask))
                wrong.append(keep(own_edge[tb], mask))
                away.append(keep(back[tb], spill))
        return [jnp.concatenate(x, axis=0) for x in (found, wrong, away)]

    def fix_pair(p):
        found, wrong, away = [
            jnp.concatenate(x, axis=1) for x in zip(fix_taps(p), fix_taps(p + 1))
        ]
        grads = jnp.concatenate([gedge[p], gedge[p + 1]], axis=1)
        z = jnp.dot(w_out_edge, found, preferred_element_type=f32) - jnp.dot(
            w_out_edge, wrong, preferred_element_type=f32
        )
        lanes = (((1,), (1,)), ((), ()))
        kedge[...] += lax.dot_general(
            found, grads, lanes, preferred_element_type=f32
        ) - lax.dot_general(wrong, grads, lanes, preferred_element_type=f32)
        da = jnp.dot(w_in_edge, away, preferred_element_type=f32)
        for w in range(2):
            held[n + p + w, :ch, :] = z[:, w * n : (w + 1) * n]
            dfix[p + w] = da[:, w * n : (w + 1) * n].reshape(sub, 8, n)

    def fix_step(g, carry):
        for w in range(4):
            fix_pair(8 * g + 2 * w)
        return carry

    lax.fori_loop(0, SLOT // 8, fix_step, 0)
    fixes_out = pltpu.make_async_copy(
        held.at[pl.ds(n, SLOT)], held_hbm.at[pl.ds(n, SLOT)], sems.at[4]
    )
    fixes_out.start()

    for y in range(2 * extra):
        i = y - extra if y < extra else n + y - extra
        ta = 0 if y < extra else 2
        e = small(((lane16 - i + EDGE) & (n - 1)) - EDGE)
        parts = []
        for tb in range(3):
            s = tb - ta
            x = grd[i + (1 - ta) * r + 2 * extra, tb * ch : (tb + 1) * ch, :]
            if s > 0:
                parts.append(keep(x, (e >= zero) & (e < reach[s])))
            elif s < 0:
                parts.append(keep(x, (e >= reach[s]) & (e < zero)))
        first = 1 if ta == 0 else 6
        weights = w_in[:, first * ch : (first + 2) * ch]
        da = jnp.dot(weights, jnp.concatenate(parts, axis=0), preferred_element_type=f32)
        dfix[SLOT + y] = da.reshape(sub, 8, n)

    kacc[...] = jnp.zeros(kacc.shape, f32)
    accs[...] = jnp.zeros(accs.shape, f32)
    def back_rows(i):
        both = two_rows(grd, i + 2 * extra, -r)
        da = jnp.dot(w_in, both, preferred_element_type=f32)
        return [da[:, w * n : (w + 1) * n].reshape(sub, 8, n) for w in range(2)]

    def kernel_part(i):
        both = jnp.concatenate([act[i + extra], act[i + extra + 1]], axis=1)
        grads = [
            jnp.concatenate(
                [grd[i + w + t * r + 2 * extra, ch : 2 * ch, :] for t in (1, 0, -1)], axis=0
            )
            for w in range(2)
        ]
        return lax.dot_general(
            both, jnp.concatenate(grads, axis=1), (((1,), (1,)), ((), ())),
            preferred_element_type=f32,
        )

    def back_step(g, carry):
        base = pl.multiple_of(g * BACK, BACK)
        total = None
        racc, c0, c1, bacc = accs[1], accs[4], accs[5], accs[7]
        for u in range(0, BACK, 2):
            i = base + u
            part = kernel_part(i)
            total = part if total is None else total + part
            for w, da in enumerate(back_rows(i)):
                slot = ((lane8 - (i + w) + EDGE) & (n - 1)) < SLOT
                da = da - jnp.where(slot[None], dfix[(u + w) % SLOT], 0.0)
                gg = grd[i + w + 2 * extra, ch : 2 * ch, :].astype(f32).reshape(sub, 8, n)
                bacc = bacc + gg
                dx = gg + slope[i + w + extra] * da
                racc = racc + jnp.where(
                    (lane8 == i + w)[None], jnp.sum(dx, axis=2, keepdims=True), 0.0
                )
                here = (lane8 >= i + w)[None]
                c0 = c0 + jnp.where(here, dx, 0.0)
                c1 = c1 + jnp.where(here, 0.0, dx)
        accs[1], accs[4], accs[5], accs[7] = racc, c0, c1, bacc
        kacc[...] += total
        return carry

    lax.fori_loop(0, n // BACK, back_step, 0)

    def add_columns(dx, t):
        for b in range(4):
            accs[3 + b] += jnp.where((t == b - 1)[None], dx, 0.0)

    def near_sums(y0):
        i0 = near_row(y0)
        which = jnp.where(y0 < extra, 0, 2)
        for w, da in enumerate(back_rows(i0)):
            i = i0 + w
            e, d = near_lanes(i)
            fix = dfix[SLOT + y0 + w]
            inner = slope[i + extra] * (da - fix)
            outer = slope[xhalo + y0 + w] * fix
            add_columns(inner, (i + ((lane8 - i) & (n - 1))) >> 7)
            add_columns(outer, (i + d) >> 7)
            total = jnp.sum(inner + outer, axis=2, keepdims=True)
            accs[which] += jnp.where((lane8 == (i & (n - 1)))[None], total, 0.0)
        return kernel_part(i0)

    def near_pair(g, carry):
        kacc[...] += near_sums(4 * g) + near_sums(4 * g + 2)
        return carry

    lax.fori_loop(0, extra // 2, near_pair, 0)

    def pack_sums(g, carry):
        for two in range(4):
            dxs = []
            for w in range(2):
                p = 8 * g + 2 * two + w
                row, e = pack_lanes(lane8, p)
                dx = slope[packs + p] * dfix[p]
                add_columns(dx, (row + jnp.where(e < 0, e, e + n)) >> 7)
                dxs.append(dx.reshape(ch, n))
            rest = jnp.concatenate(dxs, axis=1)
            parts = []
            for _ in range(3):
                part = rest.astype(bf16)
                rest = rest - part.astype(f32)
                parts.append(part)
            found = lax.dot_general(
                jnp.concatenate(parts, axis=0), place[4 * g + two],
                (((1,), (1,)), ((), ())), preferred_element_type=f32,
            )
            total = found[:ch] + found[ch : 2 * ch] + found[2 * ch :]
            accs[1] += total.reshape(sub, 8, n)
        return carry

    lax.fori_loop(0, SLOT // 8, pack_sums, 0)

    half_blocks = blocks // 2
    mine = r_id // half_blocks
    kept[...] = jnp.zeros(kept.shape, f32)
    sent[...] = jnp.zeros(sent.shape, f32)

    def put(at, first, value):
        which = jnp.where(at >= half_blocks, 1, 0)
        slot = pl.multiple_of((at - which * half_blocks) * 2 * ch + first, ch)

        @pl.when((at >= 0) & (at < blocks) & (which == mine))
        def _():
            kept[pl.ds(slot, ch), :] = value

        @pl.when((at >= 0) & (at < blocks) & (which != mine))
        def _():
            sent[pl.ds(slot, ch), :] = value

    for t in range(3):
        put(r_id + t - 1, 0, accs[t].reshape(ch, n))
    for t in range(4):
        put(r_id + k_id + t - 1, ch, accs[3 + t].reshape(ch, n))

    parts = []
    for ta in range(3):
        part = kacc[:, ta * ch : (ta + 1) * ch]
        fixes = [
            kedge[crossing.index((ta, tb)) * ch : (crossing.index((ta, tb)) + 1) * ch, :]
            if ta != tb
            else jnp.zeros((ch, ch), f32)
            for tb in range(3)
        ]
        parts.append(part + jnp.concatenate(fixes, axis=0))
    full = jnp.concatenate(parts, axis=0).T
    full = jnp.concatenate([full, jnp.zeros((ch, 3 * n - 9 * ch), f32)], axis=1)
    lanes = lax.broadcasted_iota(jnp.int32, (ch, 3 * n), 1)
    btotal = jnp.sum(accs[7].reshape(ch, n), axis=1, keepdims=True)
    full = jnp.where(lanes == 9 * ch, btotal, full)
    for t in range(3):
        first = half_blocks * 2 * ch + t * ch
        sent[first : first + ch, :] = full[:, t * n : (t + 1) * n]
    held_out.wait()
    act_out.wait()
    fixes_out.wait()


def rows_of(ref, at, step):
    return jnp.concatenate([ref[at - step], ref[at], ref[at + step]], axis=0)


def two_rows(ref, at, step):
    return jnp.concatenate([rows_of(ref, at, step), rows_of(ref, at + 1, step)], axis=1)


def out_kernel(
    start, count, weights_hbm, bias_hbm, dil_hbm, act_hbm, held_hbm, *refs
):
    pair_out, weights, bias, act, held, done, dil, sems, act_sems, held_sems, done_sems = refs[-11:]
    f32, bf16 = jnp.float32, jnp.bfloat16
    ch, n = pair_out.shape[:2]
    sub = ch // 8

    def part(hbm, vmem, sem, first, there):
        rows = pl.ds(pl.multiple_of(first, 16), 16)
        return pltpu.make_async_copy(hbm.at[rows], vmem.at[pl.ds(there, 16)], sem)

    def act_part(g):
        return part(act_hbm, act, act_sems.at[g], (start + g) * 16, g * 16)

    def held_part(g):
        return part(held_hbm, held, held_sems.at[g], (start + g) * 16, g * 16)

    def done_part(g):
        rows = pl.ds(pl.multiple_of((start + g) * 16, 16), 16)
        return pltpu.make_async_copy(done.at[g], pair_out.at[:, rows, :], done_sems.at[g])

    fixes = part(held_hbm, held, held_sems.at[count], n, count * 16)
    small = [
        pltpu.make_async_copy(a, b, sems.at[j])
        for j, (a, b) in enumerate(
            ((dil_hbm, dil), (bias_hbm, bias), (weights_hbm.at[0], weights))
        )
    ]
    for copy in small:
        copy.start()
    fixes.start()
    act_part(0).start()
    for g in range(count):
        act_part(g + 1).start()
        held_part(g).start()
    lane8 = lax.broadcasted_iota(jnp.int32, (8, n), 1)
    for copy in small:
        copy.wait()
    w_out = weights[...]
    square = [lax.broadcasted_iota(jnp.int32, (ch, ch), x) for x in range(2)]
    shift_by = jnp.sum(
        jnp.where(square[0] == square[1], jnp.broadcast_to(bias[...], (ch, ch)), 0.0),
        axis=1, keepdims=True,
    )
    shift_by = jnp.broadcast_to(shift_by, (ch, n)).reshape(sub, 8, n)
    r = jnp.max(dil[...])
    fixes.wait()
    act_part(0).wait()

    def conv_step(g, carry):
        act_part(g + 1).wait()
        held_part(g).wait()
        found = []
        for u in range(0, 16, 2):
            k = g * 16 + u
            i = start * 16 + k
            z = jnp.dot(w_out, two_rows(act, k + MAXDIL, r), preferred_element_type=f32)
            for w in range(2):
                slot = ((lane8 - (i + w) + EDGE) & (n - 1)) < SLOT
                fix = held[count * 16 + u + w, :ch, :].reshape(sub, 8, n)
                y = (held[k + w, :ch, :] + z[:, w * n : (w + 1) * n]).reshape(sub, 8, n)
                y = y + shift_by + jnp.where(slot[None], fix, 0.0)
                y = (y * held[k + w, ch:, :][None]).reshape(ch, n).astype(bf16)
                found.append(pltpu.roll(y, (n - i - w) & (n - 1), 1))
        done[g] = jnp.swapaxes(jnp.stack(found), 0, 1)
        done_part(g).start()
        return carry

    lax.fori_loop(0, count, conv_step, 0)
    for g in range(count):
        done_part(g).wait()


def out_call(start, count, made, weights, bias, dil, act, held):
    _, ch3, n = act.shape
    ch = ch3 // 3
    hbm = pl.BlockSpec(memory_space=pltpu.HBM)
    dma = pltpu.SemaphoreType.DMA

    def body(*refs):
        out_kernel(start, count, *refs)

    return pl.pallas_call(
        body,
        out_shape=jax.ShapeDtypeStruct((ch, n, n), jnp.bfloat16),
        in_specs=[hbm] * (5 + len(made)),
        out_specs=hbm,
        input_output_aliases={5: 0} if made else {},
        scratch_shapes=[
            pltpu.VMEM(weights.shape[1:], weights.dtype),
            pltpu.VMEM((1, ch), jnp.float32),
            pltpu.VMEM((16 * (count + 1), ch3, n), act.dtype),
            pltpu.VMEM((16 * (count + 1), ch + 8, n), held.dtype),
            pltpu.VMEM((count, ch, 16, n), jnp.bfloat16),
            pltpu.VMEM((1, 1), jnp.int32),
            dma((3,)),
            dma((count + 1,)),
            dma((count + 1,)),
            dma((count,)),
        ],
        compiler_params=pltpu.CompilerParams(vmem_limit_bytes=OUT_LIMIT),
        cost_estimate=pl.CostEstimate(
            flops=288 * count * ch * ch * n, bytes_accessed=200 * count * ch * n, transcendentals=0
        ),
        name="outputs",
    )(weights, bias.reshape(1, ch), dil.reshape(1, 1), act, held, *made)


def tile_call(gathered, weights, cot):
    blocks, _, n = gathered.shape
    ch = cot.shape[0]
    assert blocks % 2 == 0
    sub = ch // 8
    f32, bf16 = jnp.float32, jnp.bfloat16
    vmem = pl.BlockSpec(memory_space=pltpu.VMEM)
    hbm = pl.BlockSpec(memory_space=pltpu.HBM)
    near = 2 * MAXDIL
    units = n + 2 * near + SLOT
    return pl.pallas_call(
        tile_kernel,
        out_shape=(
            jax.ShapeDtypeStruct((blocks * ch, n), f32),
            jax.ShapeDtypeStruct((blocks * ch + 3 * ch, n), f32),
            jax.ShapeDtypeStruct((n + SLOT, 3 * ch, n), bf16),
            jax.ShapeDtypeStruct((n + SLOT, ch + 8, n), f32),
        ),
        in_specs=[vmem, hbm, hbm],
        out_specs=(vmem, vmem, hbm, hbm),
        scratch_shapes=[
            pltpu.VMEM((n + SLOT, 3 * ch, n), bf16),
            pltpu.VMEM((n + SLOT, ch + 8, n), f32),
            pltpu.VMEM((n + 2 * near, 3 * ch, n), bf16),
            pltpu.VMEM((units, sub, 8, n), f32),
            pltpu.VMEM((SLOT + near, ch, n), bf16),
            pltpu.VMEM((SLOT + near, ch, n), bf16),
            pltpu.VMEM((SLOT, ch, n), bf16),
            pltpu.VMEM((SLOT + near, sub, 8, n), f32),
            pltpu.VMEM((4, sub, 8, n), f32),
            pltpu.VMEM((4, 8, n), f32),
            pltpu.VMEM((8, sub, 8, n), f32),
            pltpu.VMEM((3 * ch, 3 * ch), f32),
            pltpu.VMEM((6 * ch, ch), f32),
            pltpu.VMEM((SLOT // 2, n, 2 * n), bf16),
            pltpu.VMEM((near, sub + 1, 8, n), f32),
            pltpu.VMEM((n, ch + 8, n), f32),
            pltpu.VMEM((ch, n, n), bf16),
            pltpu.VMEM((4, ch, 9 * ch), bf16),
            pltpu.SemaphoreType.DMA((5,)),
        ],
        compiler_params=pltpu.CompilerParams(vmem_limit_bytes=VMEM_LIMIT),
        cost_estimate=pl.CostEstimate(
            flops=54 * ch * ch * n * n, bytes_accessed=16 * ch * n * n, transcendentals=ch * n * n
        ),
        name="tile",
    )(gathered, weights, cot)


def final_kernel(scales, x, y, rows, cols, kgrad, bgrad):
    ch = rows.shape[0]
    n = rows.shape[1]
    total = x[...] + y[...]
    rows[...] = total[:ch] * scales[0]
    cols[...] = total[ch : 2 * ch] * scales[0]
    total = total[2 * ch :] * scales[1]
    for t in range(9):
        first, lane = (t * ch // n) * ch, t * ch % n
        kgrad[t] = total[first : first + ch, lane : lane + ch]
    first, lane = (9 * ch // n) * ch, 9 * ch % n
    part = jnp.broadcast_to(total[first : first + ch, lane : lane + 1], (ch, ch))
    square = [lax.broadcasted_iota(jnp.int32, (ch, ch), i) for i in range(2)]
    bgrad[...] = jnp.sum(jnp.where(square[0] == square[1], part, 0.0), axis=0, keepdims=True)


def final_call(x, y, embed_scale, weight_scale):
    n = x.shape[1]
    ch = x.shape[0] // 5
    f32 = jnp.float32

    def body(*refs):
        final_kernel((embed_scale, weight_scale), *refs)

    vmem = pl.BlockSpec(memory_space=pltpu.VMEM)
    return pl.pallas_call(
        body,
        out_shape=(
            jax.ShapeDtypeStruct((ch, n), f32),
            jax.ShapeDtypeStruct((ch, n), f32),
            jax.ShapeDtypeStruct((9, ch, ch), f32),
            jax.ShapeDtypeStruct((1, ch), f32),
        ),
        in_specs=[vmem, vmem],
        out_specs=(vmem,) * 4,
        compiler_params=pltpu.CompilerParams(vmem_limit_bytes=2 * 1024 * 1024),
        name="finish",
    )(x, y)


def swapped(value, axis, bit):
    return lax.ppermute(value, axis, [(i, i ^ bit) for i in range(lax.axis_size(axis))])


def local(emb_rows, emb_cols, kernel, bias, cotangent, valid, dilation, band):
    ch, n = emb_rows.shape
    row_devices, diag_devices = lax.axis_size("row"), lax.axis_size("diag")
    assert cotangent.shape[2] == n == 128
    assert row_devices & (row_devices - 1) == 0 and diag_devices & (diag_devices - 1) == 0
    total_diags = n * diag_devices
    bins, weights = pack_call(emb_cols, emb_rows, valid, dilation, band, kernel)
    gathered = lax.all_gather(bins, "row")
    kept, sent, *held = tile_call(gathered, weights, cotangent)
    groups = n // 16
    cut = groups - groups * 3 // 8
    made = ()

    place = lax.axis_index("row")
    bit = row_devices // 2
    while True:
        came = swapped(sent, "row", bit)
        if not made:
            made = (out_call(0, cut, (), weights, bias, dilation, *held),)
            came, *made = lax.optimization_barrier((came, *made))
        own = bit * 2 * ch
        sums, whole = kept + came[:own], sent[own:] + came[own:]
        bit //= 2
        if not bit:
            break
        halves = sums.reshape(2, bit * 2 * ch, n)
        mine = (place // bit) & 1
        kept = lax.dynamic_index_in_dim(halves, mine, 0, False)
        other = lax.dynamic_index_in_dim(halves, 1 - mine, 0, False)
        sent = jnp.concatenate([other, whole], axis=0)
    both = jnp.concatenate([sums, whole], axis=0)
    bit = 1
    while 2 * bit < diag_devices:
        both = both + swapped(both, "diag", bit)
        bit *= 2
    came = swapped(both, "diag", bit)
    pair_out = out_call(cut, groups - cut, tuple(made), weights, bias, dilation, *held)
    came, pair_out = lax.optimization_barrier((came, pair_out))
    rows, cols, kgrad, bgrad = final_call(
        both,
        came,
        1.0 / total_diags**0.5,
        1.0 / (row_devices * n * total_diags) ** 0.5,
    )
    return pair_out, rows, cols, kgrad.reshape(3, 3, ch, ch), bgrad.reshape(ch)


def solution(mesh):
    in_specs = (
        P(None, ("grp", "row")),
        P(None, ("grp", "row")),
        P(),
        P(),
        P(None, ("grp", "row"), "diag"),
        P(("grp", "row")),
        P("grp"),
        P("grp"),
    )
    out_specs = (
        P(None, ("grp", "row"), "diag"),
        P(None, ("grp", "row")),
        P(None, ("grp", "row")),
        P("grp", None, None, None),
        P("grp"),
    )
    return jax.shard_map(local, mesh=mesh, in_specs=in_specs, out_specs=out_specs, check_vma=False)
```

```python
import functools

import jax
import jax.numpy as jnp
from jax import lax
from jax.experimental import pallas as pl
from jax.experimental.pallas import tpu as pltpu
from jax.sharding import PartitionSpec as P

MAXDIL = 4
BACK = 64
EDGE = 2 * MAXDIL
SLOT = 2 * EDGE
GELU_C = 0.7978845608028654
GELU_A = 0.044715
WORD_BITS = 6
VMEM_LIMIT = 54600 * 1024
OUT_LIMIT = (65472 - 1500) * 1024


def gelu_and_slope(h):
    square = h * h
    t = jnp.tanh(h * (GELU_C + (GELU_C * GELU_A) * square))
    half = 0.5 * h
    one = 1.0 + t
    slope = 0.5 * one + half * (1.0 - t * t) * (GELU_C + (3.0 * GELU_C * GELU_A) * square)
    return half * one, slope


def crossings():
    return [(ta, tb) for ta in range(3) for tb in range(3) if ta != tb]


def pack_kernel(emb_cols, emb_rows, valid, dil, band, kernel, bias, bins, weights):
    f32, bf16 = jnp.float32, jnp.bfloat16
    ch, n = emb_cols.shape
    bins[:ch] = emb_cols[...]
    bins[ch : 2 * ch] = emb_rows[...]
    known = jnp.broadcast_to(valid[...].astype(f32), (8, n))
    wide = jnp.broadcast_to(band[...], (8, n))
    line = lax.broadcasted_iota(jnp.int32, (8, n), 0)
    settings = jnp.where(line == 1, wide >> WORD_BITS, wide & (2**WORD_BITS - 1))
    settings = jnp.where(line == 0, jnp.broadcast_to(dil[...], (8, n)), settings)
    bins[2 * ch :] = jnp.concatenate([known, settings.astype(f32)], axis=0).astype(bf16)
    taps = [kernel[t // 3, t % 3] for t in range(9)]
    turned = [w.astype(f32).T.astype(bf16) for w in taps]
    cross = [3 * ta + tb for ta, tb in crossings()]
    weights[0] = jnp.concatenate(taps, axis=1)
    weights[1] = jnp.concatenate(turned, axis=1)
    weights[2, :, : 6 * ch] = jnp.concatenate([taps[t] for t in cross], axis=1)
    weights[3, :, : 6 * ch] = jnp.concatenate([turned[t] for t in cross], axis=1)
    square = [lax.broadcasted_iota(jnp.int32, (ch, ch), x) for x in range(2)]
    rest = jnp.sum(
        jnp.where(square[0] == square[1], jnp.broadcast_to(bias[...], (ch, ch)), 0.0),
        axis=1, keepdims=True,
    )
    lane = lax.broadcasted_iota(jnp.int32, (ch, 9 * ch), 1)
    whole = jnp.zeros((ch, 9 * ch), f32)
    for j in range(3):
        part = rest.astype(bf16).astype(f32)
        rest = rest - part
        whole = jnp.where(lane == j, part, whole)
    weights[4] = whole.astype(bf16)


def pack_call(emb_cols, emb_rows, valid, dil, band, kernel, bias):
    ch, n = emb_cols.shape
    vmem = pl.BlockSpec(memory_space=pltpu.VMEM)
    return pl.pallas_call(
        pack_kernel,
        out_shape=(
            jax.ShapeDtypeStruct((2 * ch + 16, n), jnp.bfloat16),
            jax.ShapeDtypeStruct((16, ch, 9 * ch), jnp.bfloat16),
        ),
        in_specs=[vmem] * 7,
        out_specs=(vmem, vmem),
        compiler_params=pltpu.CompilerParams(vmem_limit_bytes=65472 * 1024),
        name="pack",
    )(
        emb_cols, emb_rows, valid.reshape(1, n), dil.reshape(1, 1), band.reshape(1, 1), kernel,
        bias.reshape(1, ch),
    )


def tile_kernel(
    here, gathered, weights_hbm, cot_hbm,
    kept, sent, act_hbm, held_hbm, pair_out,
    act, held, grd, slope, halo, edge, gedge, dfix, cols, colv, accs, kacc, kedge,
    place, nears, spreads, cot, weights, done, sems, done_sems,
):
    cot_in = pltpu.make_async_copy(cot_hbm, cot, sems.at[0])
    cot_in.start()
    weights_in = pltpu.make_async_copy(weights_hbm.at[pl.ds(0, 5)], weights, sems.at[1])
    weights_in.start()
    ch = cot.shape[0]
    n = cot.shape[1]
    sub = ch // 8
    blocks = gathered.shape[0]
    extra = MAXDIL
    ext = n + 2 * extra
    packs = ext
    xhalo = ext + SLOT
    r_id = lax.axis_index("row")
    k_id = lax.axis_index("diag")
    settings = gathered[r_id, 2 * ch + 8 : 2 * ch + 16, :].astype(jnp.float32)
    r, high, rest = [jnp.max(settings[j : j + 1, :]).astype(jnp.int32) for j in range(3)]
    width = (high << WORD_BITS) + rest - k_id * n
    low = -k_id * n
    f32, bf16 = jnp.float32, jnp.bfloat16
    lane8 = lax.broadcasted_iota(jnp.int32, (8, n), 1)
    lane16 = lax.broadcasted_iota(jnp.int32, (16, n), 1)

    def small(x):
        return x.astype(f32).astype(bf16)

    reach = {s: small(s * r) for s in (1, 2, -1, -2)}
    zero = jnp.array(0, bf16)

    def block_of(index, first, count):
        found = gathered[jnp.clip(index, 0, blocks - 1), first : first + count, :]
        inside = ((index >= 0) & (index < blocks)).astype(f32)
        return found.astype(f32) * inside

    for t in range(4):
        cols[t] = block_of(r_id + k_id + t - 1, 0, ch).reshape(sub, 8, n)
        colv[t] = block_of(r_id + k_id + t - 1, 2 * ch, 8)

    tall = ch + 16

    def row_values(index):
        return block_of(index, ch, tall)

    own = row_values(r_id)
    own16 = own.astype(bf16)
    sublane = lax.broadcasted_iota(jnp.int32, (16, n), 0)
    ones = [(sublane == u).astype(f32).astype(bf16) for u in range(16)]
    ones = jnp.concatenate(ones, axis=1)

    def spread16(rows):
        wide = jnp.dot(rows[:, :16], ones, preferred_element_type=f32)
        parts = [wide[:, u * n : (u + 1) * n] for u in range(16)]
        return [(x[:ch].reshape(sub, 8, n), x[ch : ch + 8]) for x in parts]

    def unit(slot, rows, rows_v, col, col_v, inside):
        v = jnp.where(inside, rows_v * col_v, 0.0)
        h = (rows + col) * v[None]
        a, g = gelu_and_slope(h)
        slope[slot] = g * v[None]
        return v, h, a.reshape(ch, n).astype(bf16)

    def pick(t):
        col, col_v = cols[3], colv[3]
        for b in (2, 1, 0):
            here = t == b - 1
            col = jnp.where(here[None], cols[b], col)
            col_v = jnp.where(here, colv[b], col_v)
        return col, col_v

    def half(x):
        return x.reshape(2, 16, n)

    def keep(x, mask):
        return jnp.where(mask[None], half(x), jnp.zeros((2, 16, n), bf16)).reshape(ch, n)

    def turns(x, back):
        ahead, behind = pltpu.roll(x, r, 1), pltpu.roll(x, n - r, 1)
        return (behind, x, ahead) if back else (ahead, x, behind)

    def store_turns(ref, at, x, back):
        for tb, y in enumerate(turns(x, back)):
            ref[at, tb * ch : (tb + 1) * ch, :] = y

    def pack_lanes(lanes, p):
        loose = p + SLOT * ((lanes - p + EDGE) >> 4)
        return loose & (n - 1), lanes - loose

    lane1 = lax.broadcasted_iota(jnp.int32, (8, n), 1)
    whole = lax.broadcasted_iota(jnp.int32, (n, n), 0)

    def packs_step(g, carry):
        for two in range(4):
            p0 = 8 * g + 2 * two
            rows_at = [pack_lanes(lane1, p0 + w)[0][:1] for w in range(2)]
            to_row = jnp.concatenate(
                [(whole == x).astype(f32).astype(bf16) for x in rows_at], axis=1
            )
            place[4 * g + two] = to_row
            found = jnp.dot(own16, to_row, preferred_element_type=f32)
            for w in range(2):
                p = p0 + w
                row, e = pack_lanes(lane8, p)
                d = jnp.where(e < 0, e, e + n)
                col, col_v = pick((row + d) >> 7)
                mine = found[:, w * n : (w + 1) * n]
                _, _, a = unit(
                    packs + p, mine[:ch].reshape(sub, 8, n), mine[ch : ch + 8], col, col_v,
                    (d >= low) & (d < width),
                )
                halo[p] = a
        return carry

    lax.fori_loop(0, SLOT // 8, packs_step, 0)

    for at in list(range(2 * extra)) + list(range(n + 2 * extra, n + 4 * extra)):
        grd[at] = jnp.zeros(grd.shape[1:], bf16)

    for g in range(n // 16):
        turned = pltpu.roll(own, (n - 16 * g) % n, 1).astype(bf16) if g else own16
        wide = jnp.dot(turned[:, :16], ones, preferred_element_type=f32)
        for u in range(16):
            spreads[16 * g + u] = wide[: ch + 8, u * n : (u + 1) * n]

    def rows_step(g, carry):
        base = pl.multiple_of(g * 32, 32)
        for u in range(32):
            i = base + u
            rows, rows_v = spreads[i, :ch, :].reshape(sub, 8, n), spreads[i, ch:, :]
            here = lane8 >= i
            col = jnp.where(here[None], cols[1], cols[2])
            col_v = jnp.where(here, colv[1], colv[2])
            d = (lane8 - i) & (n - 1)
            v, h, a = unit(i + extra, rows, rows_v, col, col_v, (d >= low) & (d < width))
            held[i, :ch, :] = h.reshape(ch, n)
            held[i, ch:, :] = v
            store_turns(act, i + extra, a, False)
        return carry

    lax.fori_loop(0, n // 32, rows_step, 0)

    def grads_step(g, carry):
        base = pl.multiple_of(g * 16, 16)
        block = jnp.swapaxes(cot[:, pl.ds(base, 16), :], 0, 1)
        for u in range(16):
            i = base + u
            v = held[i, ch:, :]
            v2 = jnp.concatenate([v, v], axis=0).astype(bf16)
            x = (half(pltpu.roll(block[u], i, 1)) * v2[None]).reshape(ch, n)
            store_turns(grd, i + 2 * extra, x, True)
        return carry

    later = pl.ds(16 * here, n - 16 * here)
    held_out = pltpu.make_async_copy(held.at[later], held_hbm.at[later], sems.at[2])
    held_out.start()
    cot_in.wait()
    lax.fori_loop(0, n // 16, grads_step, 0)

    def edges_step(g, carry):
        for w in range(4):
            p = 4 * g + w
            row = small(pack_lanes(lane16, p)[0])
            a = x = jnp.zeros((2, 16, n), bf16)
            for m in range(n // SLOT):
                i = p + m * SLOT
                here = (row == small(i))[None]
                a = jnp.where(here, half(act[i + extra, ch : 2 * ch, :]), a)
                x = jnp.where(here, half(grd[i + 2 * extra, ch : 2 * ch, :]), x)
            edge[p] = a.reshape(ch, n)
            gedge[p] = x.reshape(ch, n)
        return carry

    lax.fori_loop(0, SLOT // 4, edges_step, 0)

    lane_tall = lax.broadcasted_iota(jnp.int32, (tall, n), 1)
    near = jnp.where(
        lane_tall < extra,
        pltpu.roll(row_values(r_id - 1), extra, 1),
        pltpu.roll(row_values(r_id + 1), extra, 1),
    )
    for y, (rows, rows_v) in enumerate(spread16(near.astype(bf16))[: 2 * extra]):
        nears[y, :sub] = rows
        nears[y, sub] = rows_v

    def near_row(y):
        return jnp.where(y < extra, y - extra, n + y - extra)

    def near_lanes(i):
        e = ((lane8 - i + EDGE) & (n - 1)) - EDGE
        return e, jnp.where(e < 0, e, e + n)

    def near_step(g, carry):
        for w in range(4):
            y = 4 * g + w
            i = near_row(y)
            rows, rows_v = nears[y, :sub], nears[y, sub]
            e, d = near_lanes(i)
            col, col_v = pick((i + d) >> 7)
            inside = (e < EDGE) & (d >= low) & (d < width)
            _, _, far = unit(xhalo + y, rows, rows_v, col, col_v, inside)
            d = (lane8 - i) & (n - 1)
            col, col_v = pick((i + d) >> 7)
            _, _, a = unit(i + extra, rows, rows_v, col, col_v, (d >= low) & (d < width))
            store_turns(act, i + extra, a, False)
            slot = (small((lane16 - i + EDGE) & (n - 1)) < jnp.array(SLOT, bf16))[None]
            q = i & (SLOT - 1)
            halo[SLOT + y] = jnp.where(slot, half(far), half(halo[q])).reshape(ch, n)
            edge[SLOT + y] = jnp.where(slot, half(a), half(edge[q])).reshape(ch, n)
        return carry

    lax.fori_loop(0, extra // 2, near_step, 0)
    later = pl.ds(16 * here, n + SLOT - 16 * here)
    act_out = pltpu.make_async_copy(act.at[later], act_hbm.at[later], sems.at[3])
    act_out.start()

    weights_in.wait()
    w_in = weights[1]
    w_out_edge, w_in_edge = weights[2, :, : 6 * ch], weights[3, :, : 6 * ch]
    crossing = crossings()
    kedge[...] = jnp.zeros(kedge.shape, f32)
    rows_last = small(n - r)

    def fix_taps(p):
        row, e = pack_lanes(lane16, p)
        row, e = small(row), small(e)
        found, wrong, away = [], [], []
        for ta in range(3):
            q = (p + (ta - 1) * r) & (SLOT - 1)
            at = q
            if ta == 0:
                at = jnp.where(p < r, q + extra, q)
            elif ta == 2:
                at = jnp.where(p + r >= SLOT, q + SLOT + extra, q)
            far, own_edge = turns(halo[at], False), turns(edge[at], False)
            back = turns(gedge[(p - (ta - 1) * r) & (SLOT - 1)], True)
            for tb in range(3):
                s = tb - ta
                if s == 0:
                    continue
                if s > 0:
                    mask = (e >= reach[-s]) & (e < zero)
                    spill = (e >= zero) & (e < reach[s])
                else:
                    mask = (e >= zero) & (e < reach[-s])
                    spill = (e >= reach[s]) & (e < zero)
                if ta == 0:
                    spill = spill & (row < rows_last)
                elif ta == 2:
                    spill = spill & (row >= reach[1])
                found.append(keep(far[tb], mask))
                wrong.append(keep(own_edge[tb], mask))
                away.append(keep(back[tb], spill))
        return [jnp.concatenate(x, axis=0) for x in (found, wrong, away)]

    def fix_pair(p):
        found, wrong, away = [
            jnp.concatenate(x, axis=1) for x in zip(fix_taps(p), fix_taps(p + 1))
        ]
        grads = jnp.concatenate([gedge[p], gedge[p + 1]], axis=1)
        z = jnp.dot(w_out_edge, found, preferred_element_type=f32) - jnp.dot(
            w_out_edge, wrong, preferred_element_type=f32
        )
        lanes = (((1,), (1,)), ((), ()))
        kedge[...] += lax.dot_general(
            found, grads, lanes, preferred_element_type=f32
        ) - lax.dot_general(wrong, grads, lanes, preferred_element_type=f32)
        da = jnp.dot(w_in_edge, away, preferred_element_type=f32)
        for w in range(2):
            held[n + p + w, :ch, :] = z[:, w * n : (w + 1) * n]
            dfix[p + w] = da[:, w * n : (w + 1) * n].reshape(sub, 8, n)

    def fix_step(g, carry):
        for w in range(4):
            fix_pair(8 * g + 2 * w)
        return carry

    lax.fori_loop(0, SLOT // 8, fix_step, 0)
    fixes_out = pltpu.make_async_copy(
        held.at[pl.ds(n, SLOT)], held_hbm.at[pl.ds(n, SLOT)], sems.at[4]
    )
    fixes_out.start()

    shift_by = bias_lanes(weights[4], n)
    for g in range(here):
        done[g] = output_rows(16 * g, 16 * g, n, act, held, weights[0], shift_by, r)
    done_out = [
        pltpu.make_async_copy(
            done.at[g], pair_out.at[:, pl.ds(16 * g, 16), :], done_sems.at[g]
        )
        for g in range(here)
    ]
    for copy in done_out:
        copy.start()

    for y in range(2 * extra):
        i = y - extra if y < extra else n + y - extra
        ta = 0 if y < extra else 2
        e = small(((lane16 - i + EDGE) & (n - 1)) - EDGE)
        parts = []
        for tb in range(3):
            s = tb - ta
            x = grd[i + (1 - ta) * r + 2 * extra, tb * ch : (tb + 1) * ch, :]
            if s > 0:
                parts.append(keep(x, (e >= zero) & (e < reach[s])))
            elif s < 0:
                parts.append(keep(x, (e >= reach[s]) & (e < zero)))
        first = 1 if ta == 0 else 6
        weights = w_in[:, first * ch : (first + 2) * ch]
        da = jnp.dot(weights, jnp.concatenate(parts, axis=0), preferred_element_type=f32)
        dfix[SLOT + y] = da.reshape(sub, 8, n)

    kacc[...] = jnp.zeros(kacc.shape, f32)
    accs[...] = jnp.zeros(accs.shape, f32)
    def back_rows(i):
        both = two_rows(grd, i + 2 * extra, -r)
        da = jnp.dot(w_in, both, preferred_element_type=f32)
        return [da[:, w * n : (w + 1) * n].reshape(sub, 8, n) for w in range(2)]

    def kernel_part(i):
        both = jnp.concatenate([act[i + extra], act[i + extra + 1]], axis=1)
        grads = [
            jnp.concatenate(
                [grd[i + w + t * r + 2 * extra, ch : 2 * ch, :] for t in (1, 0, -1)], axis=0
            )
            for w in range(2)
        ]
        return lax.dot_general(
            both, jnp.concatenate(grads, axis=1), (((1,), (1,)), ((), ())),
            preferred_element_type=f32,
        )

    def back_step(g, carry):
        base = pl.multiple_of(g * BACK, BACK)
        total = None
        racc, c0, c1, bacc = accs[1], accs[4], accs[5], accs[7]
        for u in range(0, BACK, 2):
            i = base + u
            part = kernel_part(i)
            total = part if total is None else total + part
            for w, da in enumerate(back_rows(i)):
                slot = ((lane8 - (i + w) + EDGE) & (n - 1)) < SLOT
                da = da - jnp.where(slot[None], dfix[(u + w) % SLOT], 0.0)
                gg = grd[i + w + 2 * extra, ch : 2 * ch, :].astype(f32).reshape(sub, 8, n)
                bacc = bacc + gg
                dx = gg + slope[i + w + extra] * da
                racc = racc + jnp.where(
                    (lane8 == i + w)[None], jnp.sum(dx, axis=2, keepdims=True), 0.0
                )
                here = (lane8 >= i + w)[None]
                c0 = c0 + jnp.where(here, dx, 0.0)
                c1 = c1 + jnp.where(here, 0.0, dx)
        accs[1], accs[4], accs[5], accs[7] = racc, c0, c1, bacc
        kacc[...] += total
        return carry

    lax.fori_loop(0, n // BACK, back_step, 0)

    def add_columns(dx, t):
        for b in range(4):
            accs[3 + b] += jnp.where((t == b - 1)[None], dx, 0.0)

    def near_sums(y0):
        i0 = near_row(y0)
        which = jnp.where(y0 < extra, 0, 2)
        for w, da in enumerate(back_rows(i0)):
            i = i0 + w
            e, d = near_lanes(i)
            fix = dfix[SLOT + y0 + w]
            inner = slope[i + extra] * (da - fix)
            outer = slope[xhalo + y0 + w] * fix
            add_columns(inner, (i + ((lane8 - i) & (n - 1))) >> 7)
            add_columns(outer, (i + d) >> 7)
            total = jnp.sum(inner + outer, axis=2, keepdims=True)
            accs[which] += jnp.where((lane8 == (i & (n - 1)))[None], total, 0.0)
        return kernel_part(i0)

    def near_pair(g, carry):
        kacc[...] += near_sums(4 * g) + near_sums(4 * g + 2)
        return carry

    lax.fori_loop(0, extra // 2, near_pair, 0)

    def pack_sums(g, carry):
        for two in range(4):
            dxs = []
            for w in range(2):
                p = 8 * g + 2 * two + w
                row, e = pack_lanes(lane8, p)
                dx = slope[packs + p] * dfix[p]
                add_columns(dx, (row + jnp.where(e < 0, e, e + n)) >> 7)
                dxs.append(dx.reshape(ch, n))
            rest = jnp.concatenate(dxs, axis=1)
            parts = []
            for _ in range(3):
                part = rest.astype(bf16)
                rest = rest - part.astype(f32)
                parts.append(part)
            found = lax.dot_general(
                jnp.concatenate(parts, axis=0), place[4 * g + two],
                (((1,), (1,)), ((), ())), preferred_element_type=f32,
            )
            total = found[:ch] + found[ch : 2 * ch] + found[2 * ch :]
            accs[1] += total.reshape(sub, 8, n)
        return carry

    lax.fori_loop(0, SLOT // 8, pack_sums, 0)

    half_blocks = blocks // 2
    mine = r_id // half_blocks
    kept[...] = jnp.zeros(kept.shape, f32)
    sent[...] = jnp.zeros(sent.shape, f32)

    def put(at, first, value):
        which = jnp.where(at >= half_blocks, 1, 0)
        slot = pl.multiple_of((at - which * half_blocks) * 2 * ch + first, ch)

        @pl.when((at >= 0) & (at < blocks) & (which == mine))
        def _():
            kept[pl.ds(slot, ch), :] = value

        @pl.when((at >= 0) & (at < blocks) & (which != mine))
        def _():
            sent[pl.ds(slot, ch), :] = value

    for t in range(3):
        put(r_id + t - 1, 0, accs[t].reshape(ch, n))
    for t in range(4):
        put(r_id + k_id + t - 1, ch, accs[3 + t].reshape(ch, n))

    parts = []
    for ta in range(3):
        part = kacc[:, ta * ch : (ta + 1) * ch]
        fixes = [
            kedge[crossing.index((ta, tb)) * ch : (crossing.index((ta, tb)) + 1) * ch, :]
            if ta != tb
            else jnp.zeros((ch, ch), f32)
            for tb in range(3)
        ]
        parts.append(part + jnp.concatenate(fixes, axis=0))
    full = jnp.concatenate(parts, axis=0).T
    full = jnp.concatenate([full, jnp.zeros((ch, 3 * n - 9 * ch), f32)], axis=1)
    lanes = lax.broadcasted_iota(jnp.int32, (ch, 3 * n), 1)
    btotal = jnp.sum(accs[7].reshape(ch, n), axis=1, keepdims=True)
    full = jnp.where(lanes == 9 * ch, btotal, full)
    for t in range(3):
        first = half_blocks * 2 * ch + t * ch
        sent[first : first + ch, :] = full[:, t * n : (t + 1) * n]
    held_out.wait()
    act_out.wait()
    fixes_out.wait()
    for copy in done_out:
        copy.wait()


def rows_of(ref, at, step):
    return jnp.concatenate([ref[at - step], ref[at], ref[at + step]], axis=0)


def two_rows(ref, at, step):
    return jnp.concatenate([rows_of(ref, at, step), rows_of(ref, at + 1, step)], axis=1)


def bias_lanes(parts, n):
    ch = parts.shape[0]
    parts = parts.astype(jnp.float32)
    column = parts[:, :1] + parts[:, 1:2] + parts[:, 2:3]
    return jnp.broadcast_to(column, (ch, n)).reshape(ch // 8, 8, n)


def output_rows(i, k, fixes, act, held, w_out, shift_by, r):
    ch, n = w_out.shape[0], act.shape[2]
    lane8 = lax.broadcasted_iota(jnp.int32, (8, n), 1)
    found = []
    for u in range(0, 16, 2):
        z = jnp.dot(
            w_out, two_rows(act, k + u + MAXDIL, r), preferred_element_type=jnp.float32
        )
        for w in range(2):
            slot = ((lane8 - (i + u + w) + EDGE) & (n - 1)) < SLOT
            fix = held[fixes + u + w, :ch, :].reshape(ch // 8, 8, n)
            y = (held[k + u + w, :ch, :] + z[:, w * n : (w + 1) * n]).reshape(ch // 8, 8, n)
            y = y + shift_by + jnp.where(slot[None], fix, 0.0)
            y = (y * held[k + u + w, ch:, :][None]).reshape(ch, n).astype(jnp.bfloat16)
            found.append(pltpu.roll(y, (n - i - u - w) & (n - 1), 1))
    return jnp.swapaxes(jnp.stack(found), 0, 1)


def out_kernel(
    start, count, weights_hbm, dil_hbm, act_hbm, held_hbm, *refs
):
    pair_out, weights, act, held, done, dil, sems, act_sems, held_sems, done_sems = refs[-10:]
    ch, n = pair_out.shape[:2]

    def part(hbm, vmem, sem, first, there):
        rows = pl.ds(pl.multiple_of(first, 16), 16)
        return pltpu.make_async_copy(hbm.at[rows], vmem.at[pl.ds(there, 16)], sem)

    def act_part(g):
        return part(act_hbm, act, act_sems.at[g], (start + g) * 16, g * 16)

    def held_part(g):
        return part(held_hbm, held, held_sems.at[g], (start + g) * 16, g * 16)

    def done_part(g):
        rows = pl.ds(pl.multiple_of((start + g) * 16, 16), 16)
        return pltpu.make_async_copy(done.at[g], pair_out.at[:, rows, :], done_sems.at[g])

    fixes = part(held_hbm, held, held_sems.at[count], n, count * 16)
    small = [
        pltpu.make_async_copy(a, b, sems.at[j])
        for j, (a, b) in enumerate(
            ((dil_hbm, dil), *((weights_hbm.at[4 * x], weights.at[x]) for x in range(2)))
        )
    ]
    for copy in small:
        copy.start()
    fixes.start()
    act_part(0).start()
    for g in range(count):
        act_part(g + 1).start()
        held_part(g).start()
    for copy in small:
        copy.wait()
    w_out = weights[0]
    shift_by = bias_lanes(weights[1], n)
    r = jnp.max(dil[...])
    fixes.wait()
    act_part(0).wait()

    def conv_step(g, carry):
        act_part(g + 1).wait()
        held_part(g).wait()
        done[g] = output_rows(
            (start + g) * 16, g * 16, count * 16, act, held, w_out, shift_by, r
        )
        done_part(g).start()
        return carry

    lax.fori_loop(0, count, conv_step, 0)
    for g in range(count):
        done_part(g).wait()


def out_call(start, count, made, weights, dil, act, held):
    _, ch3, n = act.shape
    ch = ch3 // 3
    hbm = pl.BlockSpec(memory_space=pltpu.HBM)
    dma = pltpu.SemaphoreType.DMA

    def body(*refs):
        out_kernel(start, count, *refs)

    return pl.pallas_call(
        body,
        out_shape=jax.ShapeDtypeStruct((ch, n, n), jnp.bfloat16),
        in_specs=[hbm] * (4 + len(made)),
        out_specs=hbm,
        input_output_aliases={4: 0} if made else {},
        scratch_shapes=[
            pltpu.VMEM((2,) + weights.shape[1:], weights.dtype),
            pltpu.VMEM((16 * (count + 1), ch3, n), act.dtype),
            pltpu.VMEM((16 * (count + 1), ch + 8, n), held.dtype),
            pltpu.VMEM((count, ch, 16, n), jnp.bfloat16),
            pltpu.VMEM((1, 1), jnp.int32),
            dma((3,)),
            dma((count + 1,)),
            dma((count + 1,)),
            dma((count,)),
        ],
        compiler_params=pltpu.CompilerParams(vmem_limit_bytes=OUT_LIMIT),
        cost_estimate=pl.CostEstimate(
            flops=288 * count * ch * ch * n, bytes_accessed=200 * count * ch * n, transcendentals=0
        ),
        name="outputs",
    )(weights, dil.reshape(1, 1), act, held, *made)


def tile_call(here, gathered, weights, cot):
    blocks, _, n = gathered.shape
    ch = cot.shape[0]
    assert blocks % 2 == 0
    sub = ch // 8
    f32, bf16 = jnp.float32, jnp.bfloat16
    vmem = pl.BlockSpec(memory_space=pltpu.VMEM)
    hbm = pl.BlockSpec(memory_space=pltpu.HBM)
    near = 2 * MAXDIL
    units = n + 2 * near + SLOT
    return pl.pallas_call(
        functools.partial(tile_kernel, here),
        out_shape=(
            jax.ShapeDtypeStruct((blocks * ch, n), f32),
            jax.ShapeDtypeStruct((blocks * ch + 3 * ch, n), f32),
            jax.ShapeDtypeStruct((n + SLOT, 3 * ch, n), bf16),
            jax.ShapeDtypeStruct((n + SLOT, ch + 8, n), f32),
            jax.ShapeDtypeStruct((ch, n, n), bf16),
        ),
        in_specs=[vmem, hbm, hbm],
        out_specs=(vmem, vmem, hbm, hbm, hbm),
        scratch_shapes=[
            pltpu.VMEM((n + SLOT, 3 * ch, n), bf16),
            pltpu.VMEM((n + SLOT, ch + 8, n), f32),
            pltpu.VMEM((n + 2 * near, 3 * ch, n), bf16),
            pltpu.VMEM((units, sub, 8, n), f32),
            pltpu.VMEM((SLOT + near, ch, n), bf16),
            pltpu.VMEM((SLOT + near, ch, n), bf16),
            pltpu.VMEM((SLOT, ch, n), bf16),
            pltpu.VMEM((SLOT + near, sub, 8, n), f32),
            pltpu.VMEM((4, sub, 8, n), f32),
            pltpu.VMEM((4, 8, n), f32),
            pltpu.VMEM((8, sub, 8, n), f32),
            pltpu.VMEM((3 * ch, 3 * ch), f32),
            pltpu.VMEM((6 * ch, ch), f32),
            pltpu.VMEM((SLOT // 2, n, 2 * n), bf16),
            pltpu.VMEM((near, sub + 1, 8, n), f32),
            pltpu.VMEM((n, ch + 8, n), f32),
            pltpu.VMEM((ch, n, n), bf16),
            pltpu.VMEM((5, ch, 9 * ch), bf16),
            pltpu.VMEM((here, ch, 16, n), bf16),
            pltpu.SemaphoreType.DMA((5,)),
            pltpu.SemaphoreType.DMA((here,)),
        ],
        compiler_params=pltpu.CompilerParams(vmem_limit_bytes=VMEM_LIMIT),
        cost_estimate=pl.CostEstimate(
            flops=54 * ch * ch * n * n, bytes_accessed=16 * ch * n * n, transcendentals=ch * n * n
        ),
        name="tile",
    )(gathered, weights, cot)


def final_kernel(scales, x, y, rows, cols, kgrad, bgrad):
    ch = rows.shape[0]
    n = rows.shape[1]
    total = x[...] + y[...]
    rows[...] = total[:ch] * scales[0]
    cols[...] = total[ch : 2 * ch] * scales[0]
    total = total[2 * ch :] * scales[1]
    for t in range(9):
        first, lane = (t * ch // n) * ch, t * ch % n
        kgrad[t] = total[first : first + ch, lane : lane + ch]
    first, lane = (9 * ch // n) * ch, 9 * ch % n
    part = jnp.broadcast_to(total[first : first + ch, lane : lane + 1], (ch, ch))
    square = [lax.broadcasted_iota(jnp.int32, (ch, ch), i) for i in range(2)]
    bgrad[...] = jnp.sum(jnp.where(square[0] == square[1], part, 0.0), axis=0, keepdims=True)


def final_call(x, y, embed_scale, weight_scale):
    n = x.shape[1]
    ch = x.shape[0] // 5
    f32 = jnp.float32

    def body(*refs):
        final_kernel((embed_scale, weight_scale), *refs)

    vmem = pl.BlockSpec(memory_space=pltpu.VMEM)
    return pl.pallas_call(
        body,
        out_shape=(
            jax.ShapeDtypeStruct((ch, n), f32),
            jax.ShapeDtypeStruct((ch, n), f32),
            jax.ShapeDtypeStruct((9, ch, ch), f32),
            jax.ShapeDtypeStruct((1, ch), f32),
        ),
        in_specs=[vmem, vmem],
        out_specs=(vmem,) * 4,
        compiler_params=pltpu.CompilerParams(vmem_limit_bytes=2 * 1024 * 1024),
        name="finish",
    )(x, y)


def swapped(value, axis, bit):
    return lax.ppermute(value, axis, [(i, i ^ bit) for i in range(lax.axis_size(axis))])


def local(emb_rows, emb_cols, kernel, bias, cotangent, valid, dilation, band):
    ch, n = emb_rows.shape
    row_devices, diag_devices = lax.axis_size("row"), lax.axis_size("diag")
    assert cotangent.shape[2] == n == 128
    assert row_devices & (row_devices - 1) == 0 and diag_devices & (diag_devices - 1) == 0
    total_diags = n * diag_devices
    bins, weights = pack_call(emb_cols, emb_rows, valid, dilation, band, kernel, bias)
    gathered = lax.all_gather(bins, "row")
    groups = n // 16
    here = groups * 5 // 8
    kept, sent, *held, pair_out = tile_call(here, gathered, weights, cotangent)
    made = None

    place = lax.axis_index("row")
    bit = row_devices // 2
    while True:
        came = swapped(sent, "row", bit)
        if made is None:
            made = out_call(here, groups - here, (pair_out,), weights, dilation, *held)
            came, made = lax.optimization_barrier((came, made))
        own = bit * 2 * ch
        sums, whole = kept + came[:own], sent[own:] + came[own:]
        bit //= 2
        if not bit:
            break
        halves = sums.reshape(2, bit * 2 * ch, n)
        mine = (place // bit) & 1
        kept = lax.dynamic_index_in_dim(halves, mine, 0, False)
        other = lax.dynamic_index_in_dim(halves, 1 - mine, 0, False)
        sent = jnp.concatenate([other, whole], axis=0)
    both = jnp.concatenate([sums, whole], axis=0)
    bit = 1
    while 2 * bit < diag_devices:
        both = both + swapped(both, "diag", bit)
        bit *= 2
    came = swapped(both, "diag", bit)
    rows, cols, kgrad, bgrad = final_call(
        both,
        came,
        1.0 / total_diags**0.5,
        1.0 / (row_devices * n * total_diags) ** 0.5,
    )
    return made, rows, cols, kgrad.reshape(3, 3, ch, ch), bgrad.reshape(ch)


def solution(mesh):
    in_specs = (
        P(None, ("grp", "row")),
        P(None, ("grp", "row")),
        P(),
        P(),
        P(None, ("grp", "row"), "diag"),
        P(("grp", "row")),
        P("grp"),
        P("grp"),
    )
    out_specs = (
        P(None, ("grp", "row"), "diag"),
        P(None, ("grp", "row")),
        P(None, ("grp", "row")),
        P("grp", None, None, None),
        P("grp"),
    )
    return jax.shard_map(local, mesh=mesh, in_specs=in_specs, out_specs=out_specs, check_vma=False)
```

```python
import functools

import jax
import jax.numpy as jnp
from jax import lax
from jax.experimental import pallas as pl
from jax.experimental.pallas import tpu as pltpu
from jax.sharding import PartitionSpec as P

MAXDIL = 4
BACK = 64
EDGE = 2 * MAXDIL
SLOT = 2 * EDGE
GELU_C = 0.7978845608028654
GELU_A = 0.044715
WORD_BITS = 6
VMEM_LIMIT = 54600 * 1024
OUT_LIMIT = (65472 - 1500) * 1024


def gelu_and_slope(h):
    square = h * h
    t = jnp.tanh(h * (GELU_C + (GELU_C * GELU_A) * square))
    half = 0.5 * h
    one = 1.0 + t
    slope = 0.5 * one + half * (1.0 - t * t) * (GELU_C + (3.0 * GELU_C * GELU_A) * square)
    return half * one, slope


def crossings():
    return [(ta, tb) for ta in range(3) for tb in range(3) if ta != tb]


def pack_kernel(emb_cols, emb_rows, valid, dil, band, kernel, bias, bins, weights):
    f32, bf16 = jnp.float32, jnp.bfloat16
    ch, n = emb_cols.shape
    bins[:ch] = emb_cols[...]
    bins[ch : 2 * ch] = emb_rows[...]
    known = jnp.broadcast_to(valid[...].astype(f32), (8, n))
    wide = jnp.broadcast_to(band[...], (8, n))
    line = lax.broadcasted_iota(jnp.int32, (8, n), 0)
    settings = jnp.where(line == 1, wide >> WORD_BITS, wide & (2**WORD_BITS - 1))
    settings = jnp.where(line == 0, jnp.broadcast_to(dil[...], (8, n)), settings)
    bins[2 * ch :] = jnp.concatenate([known, settings.astype(f32)], axis=0).astype(bf16)
    taps = [kernel[t // 3, t % 3] for t in range(9)]
    turned = [w.astype(f32).T.astype(bf16) for w in taps]
    cross = [3 * ta + tb for ta, tb in crossings()]
    weights[0] = jnp.concatenate(taps, axis=1)
    weights[1] = jnp.concatenate(turned, axis=1)
    weights[2, :, : 6 * ch] = jnp.concatenate([taps[t] for t in cross], axis=1)
    weights[3, :, : 6 * ch] = jnp.concatenate([turned[t] for t in cross], axis=1)
    square = [lax.broadcasted_iota(jnp.int32, (ch, ch), x) for x in range(2)]
    rest = jnp.sum(
        jnp.where(square[0] == square[1], jnp.broadcast_to(bias[...], (ch, ch)), 0.0),
        axis=1, keepdims=True,
    )
    lane = lax.broadcasted_iota(jnp.int32, (ch, 9 * ch), 1)
    whole = jnp.zeros((ch, 9 * ch), f32)
    for j in range(3):
        part = rest.astype(bf16).astype(f32)
        rest = rest - part
        whole = jnp.where(lane == j, part, whole)
    weights[4] = whole.astype(bf16)


def pack_call(emb_cols, emb_rows, valid, dil, band, kernel, bias):
    ch, n = emb_cols.shape
    vmem = pl.BlockSpec(memory_space=pltpu.VMEM)
    return pl.pallas_call(
        pack_kernel,
        out_shape=(
            jax.ShapeDtypeStruct((2 * ch + 16, n), jnp.bfloat16),
            jax.ShapeDtypeStruct((16, ch, 9 * ch), jnp.bfloat16),
        ),
        in_specs=[vmem] * 7,
        out_specs=(vmem, vmem),
        compiler_params=pltpu.CompilerParams(vmem_limit_bytes=65472 * 1024),
        name="pack",
    )(
        emb_cols, emb_rows, valid.reshape(1, n), dil.reshape(1, 1), band.reshape(1, 1), kernel,
        bias.reshape(1, ch),
    )


def tile_kernel(
    here, gathered, weights_hbm, cot_hbm,
    kept, sent, act_hbm, held_hbm, pair_out,
    act, held, grd, slope, halo, edge, gedge, dfix, cols, colv, accs, kacc, kedge,
    place, nears, spreads, cot, weights, done, sems, done_sems,
):
    cot_in = pltpu.make_async_copy(cot_hbm, cot, sems.at[0])
    cot_in.start()
    weights_in = pltpu.make_async_copy(weights_hbm.at[pl.ds(0, 5)], weights, sems.at[1])
    weights_in.start()
    ch = cot.shape[0]
    n = cot.shape[1]
    sub = ch // 8
    blocks = gathered.shape[0]
    extra = MAXDIL
    ext = n + 2 * extra
    packs = ext
    xhalo = ext + SLOT
    r_id = lax.axis_index("row")
    k_id = lax.axis_index("diag")
    settings = gathered[r_id, 2 * ch + 8 : 2 * ch + 16, :].astype(jnp.float32)
    r, high, rest = [jnp.max(settings[j : j + 1, :]).astype(jnp.int32) for j in range(3)]
    width = (high << WORD_BITS) + rest - k_id * n
    low = -k_id * n
    f32, bf16 = jnp.float32, jnp.bfloat16
    lane8 = lax.broadcasted_iota(jnp.int32, (8, n), 1)
    lane16 = lax.broadcasted_iota(jnp.int32, (16, n), 1)

    def small(x):
        return x.astype(f32).astype(bf16)

    reach = {s: small(s * r) for s in (1, 2, -1, -2)}
    zero = jnp.array(0, bf16)

    def block_of(index, first, count):
        found = gathered[jnp.clip(index, 0, blocks - 1), first : first + count, :]
        inside = ((index >= 0) & (index < blocks)).astype(f32)
        return found.astype(f32) * inside

    for t in range(4):
        cols[t] = block_of(r_id + k_id + t - 1, 0, ch).reshape(sub, 8, n)
        colv[t] = block_of(r_id + k_id + t - 1, 2 * ch, 8)

    tall = ch + 16

    def row_values(index):
        return block_of(index, ch, tall)

    own = row_values(r_id)
    own16 = own.astype(bf16)
    sublane = lax.broadcasted_iota(jnp.int32, (16, n), 0)
    ones = [(sublane == u).astype(f32).astype(bf16) for u in range(16)]
    ones = jnp.concatenate(ones, axis=1)

    def spread16(rows):
        wide = jnp.dot(rows[:, :16], ones, preferred_element_type=f32)
        parts = [wide[:, u * n : (u + 1) * n] for u in range(16)]
        return [(x[:ch].reshape(sub, 8, n), x[ch : ch + 8]) for x in parts]

    def unit(slot, rows, rows_v, col, col_v, inside):
        v = jnp.where(inside, rows_v * col_v, 0.0)
        h = (rows + col) * v[None]
        a, g = gelu_and_slope(h)
        slope[slot] = g * v[None]
        return v, h, a.reshape(ch, n).astype(bf16)

    def pick(t):
        col, col_v = cols[3], colv[3]
        for b in (2, 1, 0):
            here = t == b - 1
            col = jnp.where(here[None], cols[b], col)
            col_v = jnp.where(here, colv[b], col_v)
        return col, col_v

    def half(x):
        return x.reshape(2, 16, n)

    def keep(x, mask):
        return jnp.where(mask[None], half(x), jnp.zeros((2, 16, n), bf16)).reshape(ch, n)

    def turns(x, back):
        ahead, behind = pltpu.roll(x, r, 1), pltpu.roll(x, n - r, 1)
        return (behind, x, ahead) if back else (ahead, x, behind)

    def store_turns(ref, at, x, back):
        for tb, y in enumerate(turns(x, back)):
            ref[at, tb * ch : (tb + 1) * ch, :] = y

    def pack_lanes(lanes, p):
        loose = p + SLOT * ((lanes - p + EDGE) >> 4)
        return loose & (n - 1), lanes - loose

    lane1 = lax.broadcasted_iota(jnp.int32, (8, n), 1)
    whole = lax.broadcasted_iota(jnp.int32, (n, n), 0)

    def packs_step(g, carry):
        for two in range(4):
            p0 = 8 * g + 2 * two
            rows_at = [pack_lanes(lane1, p0 + w)[0][:1] for w in range(2)]
            to_row = jnp.concatenate(
                [(whole == x).astype(f32).astype(bf16) for x in rows_at], axis=1
            )
            place[4 * g + two] = to_row
            found = jnp.dot(own16, to_row, preferred_element_type=f32)
            for w in range(2):
                p = p0 + w
                row, e = pack_lanes(lane8, p)
                d = jnp.where(e < 0, e, e + n)
                col, col_v = pick((row + d) >> 7)
                mine = found[:, w * n : (w + 1) * n]
                _, _, a = unit(
                    packs + p, mine[:ch].reshape(sub, 8, n), mine[ch : ch + 8], col, col_v,
                    (d >= low) & (d < width),
                )
                halo[p] = a
        return carry

    lax.fori_loop(0, SLOT // 8, packs_step, 0)

    for at in list(range(2 * extra)) + list(range(n + 2 * extra, n + 4 * extra)):
        grd[at] = jnp.zeros(grd.shape[1:], bf16)

    for g in range(n // 16):
        turned = pltpu.roll(own, (n - 16 * g) % n, 1).astype(bf16) if g else own16
        wide = jnp.dot(turned[:, :16], ones, preferred_element_type=f32)
        for u in range(16):
            spreads[16 * g + u] = wide[: ch + 8, u * n : (u + 1) * n]

    def rows_step(g, carry):
        base = pl.multiple_of(g * 32, 32)
        for u in range(32):
            i = base + u
            rows, rows_v = spreads[i, :ch, :].reshape(sub, 8, n), spreads[i, ch:, :]
            here = lane8 >= i
            col = jnp.where(here[None], cols[1], cols[2])
            col_v = jnp.where(here, colv[1], colv[2])
            d = (lane8 - i) & (n - 1)
            v, h, a = unit(i + extra, rows, rows_v, col, col_v, (d >= low) & (d < width))
            held[i, :ch, :] = h.reshape(ch, n)
            held[i, ch:, :] = v
            store_turns(act, i + extra, a, False)
        return carry

    lax.fori_loop(0, n // 32, rows_step, 0)

    def grads_step(g, carry):
        base = pl.multiple_of(g * 16, 16)
        block = jnp.swapaxes(cot[:, pl.ds(base, 16), :], 0, 1)
        for u in range(16):
            i = base + u
            v = held[i, ch:, :]
            v2 = jnp.concatenate([v, v], axis=0).astype(bf16)
            x = (half(pltpu.roll(block[u], i, 1)) * v2[None]).reshape(ch, n)
            store_turns(grd, i + 2 * extra, x, True)
        return carry

    later = pl.ds(16 * here, n - 16 * here)
    held_out = pltpu.make_async_copy(held.at[later], held_hbm.at[later], sems.at[2])
    held_out.start()
    cot_in.wait()
    lax.fori_loop(0, n // 16, grads_step, 0)

    def edges_step(g, carry):
        for w in range(4):
            p = 4 * g + w
            row = small(pack_lanes(lane16, p)[0])
            a = x = jnp.zeros((2, 16, n), bf16)
            for m in range(n // SLOT):
                i = p + m * SLOT
                here = (row == small(i))[None]
                a = jnp.where(here, half(act[i + extra, ch : 2 * ch, :]), a)
                x = jnp.where(here, half(grd[i + 2 * extra, ch : 2 * ch, :]), x)
            edge[p] = a.reshape(ch, n)
            gedge[p] = x.reshape(ch, n)
        return carry

    lax.fori_loop(0, SLOT // 4, edges_step, 0)

    lane_tall = lax.broadcasted_iota(jnp.int32, (tall, n), 1)
    near = jnp.where(
        lane_tall < extra,
        pltpu.roll(row_values(r_id - 1), extra, 1),
        pltpu.roll(row_values(r_id + 1), extra, 1),
    )
    for y, (rows, rows_v) in enumerate(spread16(near.astype(bf16))[: 2 * extra]):
        nears[y, :sub] = rows
        nears[y, sub] = rows_v

    def near_row(y):
        return jnp.where(y < extra, y - extra, n + y - extra)

    def near_lanes(i):
        e = ((lane8 - i + EDGE) & (n - 1)) - EDGE
        return e, jnp.where(e < 0, e, e + n)

    def near_step(g, carry):
        for w in range(4):
            y = 4 * g + w
            i = near_row(y)
            rows, rows_v = nears[y, :sub], nears[y, sub]
            e, d = near_lanes(i)
            col, col_v = pick((i + d) >> 7)
            inside = (e < EDGE) & (d >= low) & (d < width)
            _, _, far = unit(xhalo + y, rows, rows_v, col, col_v, inside)
            d = (lane8 - i) & (n - 1)
            col, col_v = pick((i + d) >> 7)
            _, _, a = unit(i + extra, rows, rows_v, col, col_v, (d >= low) & (d < width))
            store_turns(act, i + extra, a, False)
            slot = (small((lane16 - i + EDGE) & (n - 1)) < jnp.array(SLOT, bf16))[None]
            q = i & (SLOT - 1)
            halo[SLOT + y] = jnp.where(slot, half(far), half(halo[q])).reshape(ch, n)
            edge[SLOT + y] = jnp.where(slot, half(a), half(edge[q])).reshape(ch, n)
        return carry

    lax.fori_loop(0, extra // 2, near_step, 0)
    later = pl.ds(16 * here, n + SLOT - 16 * here)
    act_out = pltpu.make_async_copy(act.at[later], act_hbm.at[later], sems.at[3])
    act_out.start()

    weights_in.wait()
    w_in = weights[1]
    w_out_edge, w_in_edge = weights[2, :, : 6 * ch], weights[3, :, : 6 * ch]
    crossing = crossings()
    kedge[...] = jnp.zeros(kedge.shape, f32)
    rows_last = small(n - r)

    def fix_taps(p):
        row, e = pack_lanes(lane16, p)
        row, e = small(row), small(e)
        found, wrong, away = [], [], []
        for ta in range(3):
            q = (p + (ta - 1) * r) & (SLOT - 1)
            at = q
            if ta == 0:
                at = jnp.where(p < r, q + extra, q)
            elif ta == 2:
                at = jnp.where(p + r >= SLOT, q + SLOT + extra, q)
            far, own_edge = turns(halo[at], False), turns(edge[at], False)
            back = turns(gedge[(p - (ta - 1) * r) & (SLOT - 1)], True)
            for tb in range(3):
                s = tb - ta
                if s == 0:
                    continue
                if s > 0:
                    mask = (e >= reach[-s]) & (e < zero)
                    spill = (e >= zero) & (e < reach[s])
                else:
                    mask = (e >= zero) & (e < reach[-s])
                    spill = (e >= reach[s]) & (e < zero)
                if ta == 0:
                    spill = spill & (row < rows_last)
                elif ta == 2:
                    spill = spill & (row >= reach[1])
                found.append(keep(far[tb], mask))
                wrong.append(keep(own_edge[tb], mask))
                away.append(keep(back[tb], spill))
        return [jnp.concatenate(x, axis=0) for x in (found, wrong, away)]

    def fix_pair(p):
        found, wrong, away = [
            jnp.concatenate(x, axis=1) for x in zip(fix_taps(p), fix_taps(p + 1))
        ]
        grads = jnp.concatenate([gedge[p], gedge[p + 1]], axis=1)
        z = jnp.dot(w_out_edge, found, preferred_element_type=f32) - jnp.dot(
            w_out_edge, wrong, preferred_element_type=f32
        )
        lanes = (((1,), (1,)), ((), ()))
        kedge[...] += lax.dot_general(
            found, grads, lanes, preferred_element_type=f32
        ) - lax.dot_general(wrong, grads, lanes, preferred_element_type=f32)
        da = jnp.dot(w_in_edge, away, preferred_element_type=f32)
        for w in range(2):
            held[n + p + w, :ch, :] = z[:, w * n : (w + 1) * n]
            dfix[p + w] = da[:, w * n : (w + 1) * n].reshape(sub, 8, n)

    def fix_step(g, carry):
        for w in range(4):
            fix_pair(8 * g + 2 * w)
        return carry

    lax.fori_loop(0, SLOT // 8, fix_step, 0)
    fixes_out = pltpu.make_async_copy(
        held.at[pl.ds(n, SLOT)], held_hbm.at[pl.ds(n, SLOT)], sems.at[4]
    )
    fixes_out.start()

    shift_by = bias_lanes(weights[4], n)
    for g in range(here):
        done[g] = output_rows(16 * g, 16 * g, n, act, held, weights[0], shift_by, r)
    done_out = [
        pltpu.make_async_copy(
            done.at[g], pair_out.at[:, pl.ds(16 * g, 16), :], done_sems.at[g]
        )
        for g in range(here)
    ]
    for copy in done_out:
        copy.start()

    for y in range(2 * extra):
        i = y - extra if y < extra else n + y - extra
        ta = 0 if y < extra else 2
        e = small(((lane16 - i + EDGE) & (n - 1)) - EDGE)
        parts = []
        for tb in range(3):
            s = tb - ta
            x = grd[i + (1 - ta) * r + 2 * extra, tb * ch : (tb + 1) * ch, :]
            if s > 0:
                parts.append(keep(x, (e >= zero) & (e < reach[s])))
            elif s < 0:
                parts.append(keep(x, (e >= reach[s]) & (e < zero)))
        first = 1 if ta == 0 else 6
        weights = w_in[:, first * ch : (first + 2) * ch]
        da = jnp.dot(weights, jnp.concatenate(parts, axis=0), preferred_element_type=f32)
        dfix[SLOT + y] = da.reshape(sub, 8, n)

    kacc[...] = jnp.zeros(kacc.shape, f32)
    accs[...] = jnp.zeros(accs.shape, f32)
    def back_rows(i):
        both = two_rows(grd, i + 2 * extra, -r)
        da = jnp.dot(w_in, both, preferred_element_type=f32)
        return [da[:, w * n : (w + 1) * n].reshape(sub, 8, n) for w in range(2)]

    def kernel_part(i):
        both = jnp.concatenate([act[i + extra], act[i + extra + 1]], axis=1)
        grads = [
            jnp.concatenate(
                [grd[i + w + t * r + 2 * extra, ch : 2 * ch, :] for t in (1, 0, -1)], axis=0
            )
            for w in range(2)
        ]
        return lax.dot_general(
            both, jnp.concatenate(grads, axis=1), (((1,), (1,)), ((), ())),
            preferred_element_type=f32,
        )

    def back_step(g, carry):
        base = pl.multiple_of(g * BACK, BACK)
        total = None
        racc, c0, c1, bacc = accs[1], accs[4], accs[5], accs[7]
        for u in range(0, BACK, 2):
            i = base + u
            part = kernel_part(i)
            total = part if total is None else total + part
            for w, da in enumerate(back_rows(i)):
                slot = ((lane8 - (i + w) + EDGE) & (n - 1)) < SLOT
                da = da - jnp.where(slot[None], dfix[(u + w) % SLOT], 0.0)
                gg = grd[i + w + 2 * extra, ch : 2 * ch, :].astype(f32).reshape(sub, 8, n)
                bacc = bacc + gg
                dx = gg + slope[i + w + extra] * da
                racc = racc + jnp.where(
                    (lane8 == i + w)[None], jnp.sum(dx, axis=2, keepdims=True), 0.0
                )
                here = (lane8 >= i + w)[None]
                c0 = c0 + jnp.where(here, dx, 0.0)
                c1 = c1 + jnp.where(here, 0.0, dx)
        accs[1], accs[4], accs[5], accs[7] = racc, c0, c1, bacc
        kacc[...] += total
        return carry

    lax.fori_loop(0, n // BACK, back_step, 0)

    def add_columns(dx, t):
        for b in range(4):
            accs[3 + b] += jnp.where((t == b - 1)[None], dx, 0.0)

    def near_sums(y0):
        i0 = near_row(y0)
        which = jnp.where(y0 < extra, 0, 2)
        for w, da in enumerate(back_rows(i0)):
            i = i0 + w
            e, d = near_lanes(i)
            fix = dfix[SLOT + y0 + w]
            inner = slope[i + extra] * (da - fix)
            outer = slope[xhalo + y0 + w] * fix
            add_columns(inner, (i + ((lane8 - i) & (n - 1))) >> 7)
            add_columns(outer, (i + d) >> 7)
            total = jnp.sum(inner + outer, axis=2, keepdims=True)
            accs[which] += jnp.where((lane8 == (i & (n - 1)))[None], total, 0.0)
        return kernel_part(i0)

    parts = [near_sums(y) for y in range(0, 2 * extra, 2)]
    kacc[...] += (parts[0] + parts[1]) + (parts[2] + parts[3])

    def pack_sums(g, carry):
        for two in range(4):
            dxs = []
            for w in range(2):
                p = 8 * g + 2 * two + w
                row, e = pack_lanes(lane8, p)
                dx = slope[packs + p] * dfix[p]
                add_columns(dx, (row + jnp.where(e < 0, e, e + n)) >> 7)
                dxs.append(dx.reshape(ch, n))
            rest = jnp.concatenate(dxs, axis=1)
            parts = []
            for _ in range(3):
                part = rest.astype(bf16)
                rest = rest - part.astype(f32)
                parts.append(part)
            found = lax.dot_general(
                jnp.concatenate(parts, axis=0), place[4 * g + two],
                (((1,), (1,)), ((), ())), preferred_element_type=f32,
            )
            total = found[:ch] + found[ch : 2 * ch] + found[2 * ch :]
            accs[1] += total.reshape(sub, 8, n)
        return carry

    lax.fori_loop(0, SLOT // 8, pack_sums, 0)

    half_blocks = blocks // 2
    mine = r_id // half_blocks
    kept[...] = jnp.zeros(kept.shape, f32)
    sent[...] = jnp.zeros(sent.shape, f32)

    def put(at, first, value):
        which = jnp.where(at >= half_blocks, 1, 0)
        slot = pl.multiple_of((at - which * half_blocks) * 2 * ch + first, ch)

        @pl.when((at >= 0) & (at < blocks) & (which == mine))
        def _():
            kept[pl.ds(slot, ch), :] = value

        @pl.when((at >= 0) & (at < blocks) & (which != mine))
        def _():
            sent[pl.ds(slot, ch), :] = value

    for t in range(3):
        put(r_id + t - 1, 0, accs[t].reshape(ch, n))
    for t in range(4):
        put(r_id + k_id + t - 1, ch, accs[3 + t].reshape(ch, n))

    parts = []
    for ta in range(3):
        part = kacc[:, ta * ch : (ta + 1) * ch]
        fixes = [
            kedge[crossing.index((ta, tb)) * ch : (crossing.index((ta, tb)) + 1) * ch, :]
            if ta != tb
            else jnp.zeros((ch, ch), f32)
            for tb in range(3)
        ]
        parts.append(part + jnp.concatenate(fixes, axis=0))
    full = jnp.concatenate(parts, axis=0).T
    full = jnp.concatenate([full, jnp.zeros((ch, 3 * n - 9 * ch), f32)], axis=1)
    lanes = lax.broadcasted_iota(jnp.int32, (ch, 3 * n), 1)
    btotal = jnp.sum(accs[7].reshape(ch, n), axis=1, keepdims=True)
    full = jnp.where(lanes == 9 * ch, btotal, full)
    for t in range(3):
        first = half_blocks * 2 * ch + t * ch
        sent[first : first + ch, :] = full[:, t * n : (t + 1) * n]
    held_out.wait()
    act_out.wait()
    fixes_out.wait()
    for copy in done_out:
        copy.wait()


def rows_of(ref, at, step):
    return jnp.concatenate([ref[at - step], ref[at], ref[at + step]], axis=0)


def two_rows(ref, at, step):
    return jnp.concatenate([rows_of(ref, at, step), rows_of(ref, at + 1, step)], axis=1)


def bias_lanes(parts, n):
    ch = parts.shape[0]
    parts = parts.astype(jnp.float32)
    column = parts[:, :1] + parts[:, 1:2] + parts[:, 2:3]
    return jnp.broadcast_to(column, (ch, n)).reshape(ch // 8, 8, n)


def output_rows(i, k, fixes, act, held, w_out, shift_by, r):
    ch, n = w_out.shape[0], act.shape[2]
    lane8 = lax.broadcasted_iota(jnp.int32, (8, n), 1)
    found = []
    for u in range(0, 16, 2):
        z = jnp.dot(
            w_out, two_rows(act, k + u + MAXDIL, r), preferred_element_type=jnp.float32
        )
        for w in range(2):
            slot = ((lane8 - (i + u + w) + EDGE) & (n - 1)) < SLOT
            fix = held[fixes + u + w, :ch, :].reshape(ch // 8, 8, n)
            y = (held[k + u + w, :ch, :] + z[:, w * n : (w + 1) * n]).reshape(ch // 8, 8, n)
            y = y + shift_by + jnp.where(slot[None], fix, 0.0)
            y = (y * held[k + u + w, ch:, :][None]).reshape(ch, n).astype(jnp.bfloat16)
            found.append(pltpu.roll(y, (n - i - u - w) & (n - 1), 1))
    return jnp.swapaxes(jnp.stack(found), 0, 1)


def out_kernel(
    start, count, weights_hbm, dil_hbm, act_hbm, held_hbm, *refs
):
    pair_out, weights, act, held, done, dil, sems, act_sems, held_sems, done_sems = refs[-10:]
    ch, n = pair_out.shape[:2]

    def part(hbm, vmem, sem, first, there):
        rows = pl.ds(pl.multiple_of(first, 16), 16)
        return pltpu.make_async_copy(hbm.at[rows], vmem.at[pl.ds(there, 16)], sem)

    def act_part(g):
        return part(act_hbm, act, act_sems.at[g], (start + g) * 16, g * 16)

    def held_part(g):
        return part(held_hbm, held, held_sems.at[g], (start + g) * 16, g * 16)

    def done_part(g):
        rows = pl.ds(pl.multiple_of((start + g) * 16, 16), 16)
        return pltpu.make_async_copy(done.at[g], pair_out.at[:, rows, :], done_sems.at[g])

    fixes = part(held_hbm, held, held_sems.at[count], n, count * 16)
    small = [
        pltpu.make_async_copy(a, b, sems.at[j])
        for j, (a, b) in enumerate(
            ((dil_hbm, dil), *((weights_hbm.at[4 * x], weights.at[x]) for x in range(2)))
        )
    ]
    for copy in small:
        copy.start()
    fixes.start()
    act_part(0).start()
    for g in range(count):
        act_part(g + 1).start()
        held_part(g).start()
    for copy in small:
        copy.wait()
    w_out = weights[0]
    shift_by = bias_lanes(weights[1], n)
    r = jnp.max(dil[...])
    fixes.wait()
    act_part(0).wait()

    def conv_step(g, carry):
        act_part(g + 1).wait()
        held_part(g).wait()
        done[g] = output_rows(
            (start + g) * 16, g * 16, count * 16, act, held, w_out, shift_by, r
        )
        done_part(g).start()
        return carry

    lax.fori_loop(0, count, conv_step, 0)
    for g in range(count):
        done_part(g).wait()


def out_call(start, count, made, weights, dil, act, held):
    _, ch3, n = act.shape
    ch = ch3 // 3
    hbm = pl.BlockSpec(memory_space=pltpu.HBM)
    dma = pltpu.SemaphoreType.DMA

    def body(*refs):
        out_kernel(start, count, *refs)

    return pl.pallas_call(
        body,
        out_shape=jax.ShapeDtypeStruct((ch, n, n), jnp.bfloat16),
        in_specs=[hbm] * (4 + len(made)),
        out_specs=hbm,
        input_output_aliases={4: 0} if made else {},
        scratch_shapes=[
            pltpu.VMEM((2,) + weights.shape[1:], weights.dtype),
            pltpu.VMEM((16 * (count + 1), ch3, n), act.dtype),
            pltpu.VMEM((16 * (count + 1), ch + 8, n), held.dtype),
            pltpu.VMEM((count, ch, 16, n), jnp.bfloat16),
            pltpu.VMEM((1, 1), jnp.int32),
            dma((3,)),
            dma((count + 1,)),
            dma((count + 1,)),
            dma((count,)),
        ],
        compiler_params=pltpu.CompilerParams(vmem_limit_bytes=OUT_LIMIT),
        cost_estimate=pl.CostEstimate(
            flops=288 * count * ch * ch * n, bytes_accessed=200 * count * ch * n, transcendentals=0
        ),
        name="outputs",
    )(weights, dil.reshape(1, 1), act, held, *made)


def tile_call(here, gathered, weights, cot):
    blocks, _, n = gathered.shape
    ch = cot.shape[0]
    assert blocks % 2 == 0
    sub = ch // 8
    f32, bf16 = jnp.float32, jnp.bfloat16
    vmem = pl.BlockSpec(memory_space=pltpu.VMEM)
    hbm = pl.BlockSpec(memory_space=pltpu.HBM)
    near = 2 * MAXDIL
    units = n + 2 * near + SLOT
    return pl.pallas_call(
        functools.partial(tile_kernel, here),
        out_shape=(
            jax.ShapeDtypeStruct((blocks * ch, n), f32),
            jax.ShapeDtypeStruct((blocks * ch + 3 * ch, n), f32),
            jax.ShapeDtypeStruct((n + SLOT, 3 * ch, n), bf16),
            jax.ShapeDtypeStruct((n + SLOT, ch + 8, n), f32),
            jax.ShapeDtypeStruct((ch, n, n), bf16),
        ),
        in_specs=[vmem, hbm, hbm],
        out_specs=(vmem, vmem, hbm, hbm, hbm),
        scratch_shapes=[
            pltpu.VMEM((n + SLOT, 3 * ch, n), bf16),
            pltpu.VMEM((n + SLOT, ch + 8, n), f32),
            pltpu.VMEM((n + 2 * near, 3 * ch, n), bf16),
            pltpu.VMEM((units, sub, 8, n), f32),
            pltpu.VMEM((SLOT + near, ch, n), bf16),
            pltpu.VMEM((SLOT + near, ch, n), bf16),
            pltpu.VMEM((SLOT, ch, n), bf16),
            pltpu.VMEM((SLOT + near, sub, 8, n), f32),
            pltpu.VMEM((4, sub, 8, n), f32),
            pltpu.VMEM((4, 8, n), f32),
            pltpu.VMEM((8, sub, 8, n), f32),
            pltpu.VMEM((3 * ch, 3 * ch), f32),
            pltpu.VMEM((6 * ch, ch), f32),
            pltpu.VMEM((SLOT // 2, n, 2 * n), bf16),
            pltpu.VMEM((near, sub + 1, 8, n), f32),
            pltpu.VMEM((n, ch + 8, n), f32),
            pltpu.VMEM((ch, n, n), bf16),
            pltpu.VMEM((5, ch, 9 * ch), bf16),
            pltpu.VMEM((here, ch, 16, n), bf16),
            pltpu.SemaphoreType.DMA((5,)),
            pltpu.SemaphoreType.DMA((here,)),
        ],
        compiler_params=pltpu.CompilerParams(vmem_limit_bytes=VMEM_LIMIT),
        cost_estimate=pl.CostEstimate(
            flops=54 * ch * ch * n * n, bytes_accessed=16 * ch * n * n, transcendentals=ch * n * n
        ),
        name="tile",
    )(gathered, weights, cot)


def final_kernel(scales, x, y, rows, cols, kgrad, bgrad):
    ch = rows.shape[0]
    n = rows.shape[1]
    total = x[...] + y[...]
    rows[...] = total[:ch] * scales[0]
    cols[...] = total[ch : 2 * ch] * scales[0]
    total = total[2 * ch :] * scales[1]
    for t in range(9):
        first, lane = (t * ch // n) * ch, t * ch % n
        kgrad[t] = total[first : first + ch, lane : lane + ch]
    first, lane = (9 * ch // n) * ch, 9 * ch % n
    part = jnp.broadcast_to(total[first : first + ch, lane : lane + 1], (ch, ch))
    square = [lax.broadcasted_iota(jnp.int32, (ch, ch), i) for i in range(2)]
    bgrad[...] = jnp.sum(jnp.where(square[0] == square[1], part, 0.0), axis=0, keepdims=True)


def final_call(x, y, embed_scale, weight_scale):
    n = x.shape[1]
    ch = x.shape[0] // 5
    f32 = jnp.float32

    def body(*refs):
        final_kernel((embed_scale, weight_scale), *refs)

    vmem = pl.BlockSpec(memory_space=pltpu.VMEM)
    return pl.pallas_call(
        body,
        out_shape=(
            jax.ShapeDtypeStruct((ch, n), f32),
            jax.ShapeDtypeStruct((ch, n), f32),
            jax.ShapeDtypeStruct((9, ch, ch), f32),
            jax.ShapeDtypeStruct((1, ch), f32),
        ),
        in_specs=[vmem, vmem],
        out_specs=(vmem,) * 4,
        compiler_params=pltpu.CompilerParams(vmem_limit_bytes=2 * 1024 * 1024),
        name="finish",
    )(x, y)


def swapped(value, axis, bit):
    return lax.ppermute(value, axis, [(i, i ^ bit) for i in range(lax.axis_size(axis))])


def local(emb_rows, emb_cols, kernel, bias, cotangent, valid, dilation, band):
    ch, n = emb_rows.shape
    row_devices, diag_devices = lax.axis_size("row"), lax.axis_size("diag")
    assert cotangent.shape[2] == n == 128
    assert row_devices & (row_devices - 1) == 0 and diag_devices & (diag_devices - 1) == 0
    total_diags = n * diag_devices
    bins, weights = pack_call(emb_cols, emb_rows, valid, dilation, band, kernel, bias)
    gathered = lax.all_gather(bins, "row")
    groups = n // 16
    here = groups * 5 // 8
    kept, sent, *held, pair_out = tile_call(here, gathered, weights, cotangent)
    made = None

    place = lax.axis_index("row")
    bit = row_devices // 2
    while True:
        came = swapped(sent, "row", bit)
        if made is None:
            made = out_call(here, groups - here, (pair_out,), weights, dilation, *held)
            came, made = lax.optimization_barrier((came, made))
        own = bit * 2 * ch
        sums, whole = kept + came[:own], sent[own:] + came[own:]
        bit //= 2
        if not bit:
            break
        halves = sums.reshape(2, bit * 2 * ch, n)
        mine = (place // bit) & 1
        kept = lax.dynamic_index_in_dim(halves, mine, 0, False)
        other = lax.dynamic_index_in_dim(halves, 1 - mine, 0, False)
        sent = jnp.concatenate([other, whole], axis=0)
    both = jnp.concatenate([sums, whole], axis=0)
    bit = 1
    while 2 * bit < diag_devices:
        both = both + swapped(both, "diag", bit)
        bit *= 2
    came = swapped(both, "diag", bit)
    rows, cols, kgrad, bgrad = final_call(
        both,
        came,
        1.0 / total_diags**0.5,
        1.0 / (row_devices * n * total_diags) ** 0.5,
    )
    return made, rows, cols, kgrad.reshape(3, 3, ch, ch), bgrad.reshape(ch)


def solution(mesh):
    in_specs = (
        P(None, ("grp", "row")),
        P(None, ("grp", "row")),
        P(),
        P(),
        P(None, ("grp", "row"), "diag"),
        P(("grp", "row")),
        P("grp"),
        P("grp"),
    )
    out_specs = (
        P(None, ("grp", "row"), "diag"),
        P(None, ("grp", "row")),
        P(None, ("grp", "row")),
        P("grp", None, None, None),
        P("grp"),
    )
    return jax.shard_map(local, mesh=mesh, in_specs=in_specs, out_specs=out_specs, check_vma=False)
```
